32 devices in a mesh: gx: 4 (over y, x), gy: 4 (over z), gz: 2 (over core).
Axes of the slice: x: 2, y: 2, z: 4, core: 2. Of those that a mesh axis runs over, the one named last changes fastest.
Arguments:
- fields: bfloat16 [4096, 2048], P(('gx', 'gy', 'gz')), may hold values from -6 to 6
- coordinates: float32 [3, 524288], P(None, ('gx', 'gy', 'gz')), may hold values from -1 to 1
- element_rank: int32 [524288, 1], P(('gx', 'gy', 'gz')), may hold values from 0 to 31; in each aligned block of 16384 rows (0 to 16383, 16384 to 32767, ...) at most 640 rows name the same one
- element_slot: int32 [524288], P(('gx', 'gy', 'gz')), may hold values from 0 to 127
Outputs:
- samples: float32 [4, 524288], P(None, ('gx', 'gy', 'gz'))
The draws below stay inside these ranges and needn't reach their ends.
Inputs may be any that keep to these rules, and one draw needn't show every extreme that they name: `element_rank`: among the probes of one device no rank is named by more than 640 probes, and in some devices' blocks one rank is named by exactly 640.
All inputs are finite; a program needn't handle non-finite values.
Results may differ from the reference program's by a relative error of at most 0.0024.
Values sent between devices are 32-bit elements; how exact they have to be, the bound alone decides.
A program may use at most 64 MiB of HBM per device.

```python
import math
import jax
import jax.numpy as jnp
import numpy as np
from jax import lax

ROW = 2048
E_DEV = 128
P_DEV = 16384
CAP = 640
ELEMENTS = 4096
PROBES = 524288
DEVICES = 32


def place_ends(values, key, least, largest):
    longest = values.shape.index(max(values.shape))
    spots = []
    for shift in (0, 1):
        where = [jax.random.randint(jax.random.fold_in(key, axis), (), 0, length) for axis, length in enumerate(values.shape)]
        where[longest] = (where[longest] + shift) % values.shape[longest]
        spots.append(tuple(where))
    return values.at[spots[0]].set(least).at[spots[1]].set(largest)


def shard_levels(rng, dims, split, least, largest):
    loudness = 1.0
    for axis_at, parts in split:
        heights = jax.random.uniform(jax.random.fold_in(jax.random.fold_in(rng, 6), axis_at), (parts,), jnp.float32, least / len(split), largest / len(split))
        loudness = loudness * jnp.repeat(jnp.exp(heights), dims[axis_at] // parts).reshape((-1,) + (1,) * (len(dims) - 1 - axis_at))
    return loudness


def routed_block(key, own, number, rows, count, top, most, slope):
    sequence = jax.random.permutation(key, count)
    packed, usual = shares(count, rows * top, most, slope, True), shares(count, rows * top, most, slope, False)
    places = jnp.arange(count)

    def named(sizes, turn):
        used = int((sizes > 0).sum())
        fixed = max(1, used // 4)
        shifted = fixed + (places - fixed + turn * (used - fixed)) % max(1, count - fixed)
        return jnp.zeros((count,), jnp.int32).at[sequence[jnp.where(places < fixed, places, shifted)]].set(jnp.asarray(sizes, jnp.int32))

    sizes = jnp.where(number % 4 == 0, named(packed, number // 4), named(usual, number - number // 4 - 1))
    mixed = jax.random.permutation(jax.random.fold_in(own, 3), count)
    source_of, sink = mixed[0:count // 2 * 2:2], mixed[1:count // 2 * 2:2]
    margin = jnp.minimum(sizes[source_of] - 1, most - sizes[sink]) // 2
    margin = jnp.where((source_of == sequence[0]) | (sink == sequence[0]) | (sizes[sink] == 0), 0, jnp.maximum(margin, 0))
    shifted = jax.random.randint(jax.random.fold_in(own, 4), (count // 2,), 0, 1 << 20) % (margin + 1)
    sizes = sizes.at[source_of].add(-shifted).at[sink].add(shifted)
    labels = jnp.searchsorted(jnp.cumsum(sizes), jnp.arange(rows * top), side="right").astype(jnp.int32)
    listing = labels.reshape(top, rows).T
    listing = listing[jax.random.permutation(jax.random.fold_in(own, 1), rows)]
    turn = jax.random.randint(jax.random.fold_in(own, 2), (rows, 1), 0, top)
    return jnp.take_along_axis(listing, (jnp.arange(top)[None, :] + turn) % top, axis=1)


def shares(count, total, bound, skew, full):
    loads = [(1 << 20) // math.isqrt(standing ** skew) + 1 for standing in range(1, count + 1)]
    largest = bound if full else min(bound, max(-(-total // count), total * loads[0] // sum(loads)))
    least = 1 if total - largest >= count - 1 else 0
    given, rest = [largest] + [least] * (count - 1), total - largest - least * (count - 1)
    while rest > 0:
        free = [i for i in range(1, count) if given[i] < largest] or [i for i in range(1, count) if given[i] < bound]
        pool, remaining = sum([loads[i] for i in free]), rest
        for i in free:
            addition = min(bound - given[i], max(1, remaining * loads[i] // pool), rest)
            given[i] = given[i] + addition
            rest = rest - addition
    return np.array(given)


def bell_draw(own_key, extent, spread, most, shards=(), held_as=jnp.bfloat16):
    drawn = jax.random.normal(own_key, extent, jnp.float32) * spread
    if len(shards) > 0:
        drawn = shard_levels(own_key, extent, shards, -0.22, 0.18) * drawn
    return jnp.clip(drawn, min=-most, max=most).astype(held_as)


def setup_inputs(seed: int = 0) -> dict:
    arg_keys = jax.random.split(jax.random.key(seed), 5)
    fields = bell_draw(arg_keys[0], (ELEMENTS, ROW), 1.0, 6.0, ((0, 32),))
    coordinates = jnp.clip(jax.random.uniform(arg_keys[1], (3, PROBES), jnp.float32, -1.0, 1.0) * shard_levels(arg_keys[1], (3, PROBES), ((1, 32),), -0.4, 0.0), -1.0, 1.0)
    element_rank_keys = jax.random.split(jax.random.fold_in(arg_keys[2], 1), PROBES // P_DEV)
    element_rank_turns = jax.random.permutation(jax.random.fold_in(arg_keys[2], 3), PROBES // P_DEV)
    element_rank = jax.vmap(lambda own, number: routed_block(jax.random.fold_in(arg_keys[2], 2), own, number, P_DEV, DEVICES, 1, CAP, 2))(element_rank_keys, element_rank_turns).reshape((PROBES, 1))
    element_slot = place_ends(jax.random.randint(arg_keys[3], (PROBES,), 0, E_DEV), jax.random.fold_in(arg_keys[3], 1), 0, E_DEV - 1).astype(jnp.int32)
    return {"fields": fields, "coordinates": coordinates, "element_rank": element_rank, "element_slot": element_slot}


gll_points = np.array([-1.0, -0.8717401485096066, -0.5917001814331423, -0.2092992179024789, 0.2092992179024789, 0.5917001814331423, 0.8717401485096066, 1.0])
gll_scale = np.array([1.0 / np.prod([gll_points[a] - gll_points[b] for b in range(8) if b != a]) for a in range(8)])


def lagrange(coord):
    offsets = coord[None, :] - jnp.asarray(gll_points, coord.dtype)[:, None]
    weights = []
    for node_a in range(8):
        factor = jnp.ones_like(coord) * gll_scale[node_a]
        for node_b in range(8):
            if node_b != node_a:
                factor = factor * offsets[node_b]
        weights.append(factor)
    return jnp.stack(weights, axis=0)


def interpolate(coordinates, element, fields):
    total_rows = element.shape[0]
    block_rows = math.gcd(total_rows, 8192)
    block_count = total_rows // block_rows

    def one_block(pieces):
        coords_block, slots_block = pieces
        weight_r = lagrange(coords_block[0])
        weight_s = lagrange(coords_block[1])
        weight_t = lagrange(coords_block[2]).astype(jnp.bfloat16)
        gathered = jnp.take(fields, slots_block, axis=0).reshape(block_rows, 256, 8)
        along_t = jnp.einsum("nak,kn->na", gathered.astype(jnp.float32), weight_t.astype(jnp.float32), precision=lax.Precision.HIGHEST)
        along_t = along_t.reshape(block_rows, 4, 8, 8)
        along_s = jnp.einsum("nfij,jn->nfi", along_t, weight_s, precision=lax.Precision.HIGHEST)
        return jnp.einsum("nfi,in->fn", along_s, weight_r, precision=lax.Precision.HIGHEST)

    coords_blocks = coordinates.reshape(3, block_count, block_rows).transpose(1, 0, 2)
    slot_blocks = element.reshape(block_count, block_rows)
    result = lax.map(one_block, (coords_blocks, slot_blocks))
    return result.transpose(1, 0, 2).reshape(4, total_rows)


def reference(fields, coordinates, element_rank, element_slot):
    element = element_rank[:, 0].astype(jnp.int32) * E_DEV + element_slot.astype(jnp.int32)
    return interpolate(coordinates, element, fields)
```

```python
import functools

import jax
import jax.numpy as jnp
import numpy as np
from jax import lax
from jax.experimental import pallas as pl
from jax.experimental.pallas import tpu as pltpu
from jax.sharding import PartitionSpec as P

AXES = ("gx", "gy", "gz")
F32, BF16 = jnp.float32, jnp.bfloat16
LANES = 128
CHUNK = 256
GROUP = 4
BATCH = 16
SWEEP = 16
STRIDE = 4

gll_points = np.array(
    [
        -1.0,
        -0.8717401485096066,
        -0.5917001814331423,
        -0.2092992179024789,
        0.2092992179024789,
        0.5917001814331423,
        0.8717401485096066,
        1.0,
    ]
)
gll_scale = np.array(
    [1.0 / np.prod([gll_points[a] - gll_points[b] for b in range(8) if b != a]) for a in range(8)]
)


def column(values):
    node = lax.broadcasted_iota(jnp.int32, (8, LANES), 0)
    out = jnp.full((8, LANES), float(values[0]), F32)
    for a in range(1, 8):
        out = jnp.where(node == a, float(values[a]), out)
    return out


def iota_bf16(shape):
    return lax.broadcasted_iota(jnp.int32, shape, 0).astype(F32).astype(BF16)


def spread(row, count):
    return jnp.broadcast_to(row, (count, row.shape[1])).astype(BF16)


def splits(count):
    groups = max(1, 2 * LANES // count)
    return groups, LANES // groups, max(1, LANES // count)


def exchange(pieces, count):
    block = lax.broadcasted_iota(jnp.int32, pieces[0].shape, 1) // count
    bit = len(pieces) // 2
    while bit:
        high = (block // bit) % 2 == 1
        swapped = []
        for i, own in enumerate(pieces):
            upper = (i // bit) % 2 == 1
            other = pltpu.roll(pieces[i - bit if upper else i + bit], LANES - bit * count if upper else bit * count, 1)
            swapped.append(jnp.where(high, own, other) if upper else jnp.where(high, other, own))
        pieces = swapped
        bit //= 2
    return pieces


def prepare(prefix_ref, nodes_ref):
    below = lax.broadcasted_iota(jnp.int32, (CHUNK, CHUNK), 0) <= lax.broadcasted_iota(jnp.int32, (CHUNK, CHUNK), 1)
    prefix_ref[:, :CHUNK] = jnp.where(below, 1.0, 0.0).astype(BF16)
    prefix_ref[:, CHUNK:] = jnp.ones((CHUNK, CHUNK), BF16)
    nodes_ref[0:8, :] = column(gll_scale)
    for k in range(1, 8):
        nodes_ref[8 * k : 8 * k + 8, :] = column(np.roll(gll_points, -k))


def turn(tile, fields_ref, turned_ref, flip_ref):
    elements = fields_ref.shape[0]
    columns = pl.ds(pl.multiple_of(tile * LANES, LANES), LANES)
    rows = pl.ds(pl.multiple_of(tile * 16, 16), 16)
    flip_ref[...] = fields_ref[:, columns].astype(F32).T
    near, nodes = elements // 2, turned_ref.shape[0] // 2
    beyond = pl.ds(pl.multiple_of(nodes + tile * 16, 16), 16)
    for c in range(0, 8, 2):
        one, two = [flip_ref[pl.ds(c + i, 16, stride=8), :] for i in range(2)]
        left = lax.broadcasted_iota(jnp.int32, one.shape, 1) < near
        turned_ref[rows, c * near : (c + 2) * near] = jnp.where(left, one, pltpu.roll(two, near, 1)).astype(BF16)
        turned_ref[beyond, c * near : (c + 2) * near] = jnp.where(left, pltpu.roll(one, near, 1), two).astype(BF16)


def place_all(count, rank_ref, prefix_ref, row_ref, lane_ref):
    probes = rank_ref.shape[1]
    group = max(1, CHUNK // count)
    groups, width, _ = splits(count)
    targets = lax.broadcasted_iota(jnp.int32, (count, CHUNK), 0)

    def place(outer, carry):
        for inner in range(STRIDE):
            step = outer * STRIDE + inner
            masks, hots, ranks = [], [], []
            for g in range(group):
                at = pl.ds(pl.multiple_of((step * group + g) * CHUNK, CHUNK), CHUNK)
                rank = rank_ref[:, at]
                mask = targets == jnp.broadcast_to(rank, (count, CHUNK))
                masks.append(mask)
                hots.append(jnp.where(mask, 1.0, 0.0).astype(BF16))
                ranks.append(rank.astype(F32))
            counted = jnp.dot(jnp.concatenate(hots, axis=0), prefix_ref[...], preferred_element_type=F32)
            for g in range(group):
                at = pl.ds(pl.multiple_of((step * group + g) * CHUNK, CHUNK), CHUNK)
                piece = counted[g * count : (g + 1) * count]
                place_in = jnp.where(masks[g], piece[:, :CHUNK] + carry, 0.0)
                position = jnp.sum(place_in, axis=0, keepdims=True) - 1.0
                part = jnp.floor(position * (1.0 / width))
                block = jnp.floor(part * (1.0 / groups))
                lane_ref[:, at] = position - (part - block) * width
                row_ref[:, at] = (part - block * groups) * count + ranks[g]
                carry = carry + piece[:, CHUNK:]
        return carry

    lax.fori_loop(0, probes // (CHUNK * group * STRIDE), place, jnp.zeros((count, CHUNK), F32))


def route(count, blocks, coords_ref, slot_ref, fields_ref, turned_ref, flip_ref, send_ref, row_ref, lane_ref, acc_ref):
    probes = slot_ref.shape[1]
    groups, width, per = splits(count)
    rows = groups * count
    spots = blocks * width
    tiles = fields_ref.shape[1] // LANES
    steps = probes // (BATCH * CHUNK)
    row_ids = iota_bf16((rows, CHUNK))
    lane_ids = iota_bf16((spots, CHUNK))
    one, zero = jnp.ones((), BF16), jnp.zeros((), BF16)
    acc_ref[...] = jnp.zeros_like(acc_ref)

    def scatter(step, _):
        row_hots, lane_parts = [], []
        for g in range(BATCH):
            at = pl.ds(pl.multiple_of((step * BATCH + g) * CHUNK, CHUNK), CHUNK)
            row_hots.append(jnp.where(row_ids == spread(row_ref[:, at], rows), one, zero))
            here = lane_ids == spread(lane_ref[:, at], spots)
            parts = []
            for v in range(3):
                value = coords_ref[v : v + 1, at]
                high = value.astype(BF16).astype(F32)
                parts += [high, value - high]
            parts.append(slot_ref[:, at].astype(F32))
            lane_parts.append(jnp.concatenate([jnp.where(here, spread(part, spots), zero) for part in parts], axis=0))
        acc_ref[...] += lax.dot_general(
            jnp.concatenate(lane_parts, axis=1),
            jnp.concatenate(row_hots, axis=1),
            (((1,), (1,)), ((), ())),
            preferred_element_type=F32,
        )
        for tile in range(tiles // steps):
            turn(step * (tiles // steps) + tile, fields_ref, turned_ref, flip_ref)
        return 0

    lax.fori_loop(0, steps, scatter, 0)
    for b in range(blocks):
        for first in range(0, 4, per):
            stacked = []
            for half in range(groups // per):
                columns = slice(half * LANES, (half + 1) * LANES)
                pieces = []
                for v in range(first, first + per):
                    at = 2 * v * spots + b * width
                    piece = acc_ref[at : at + width, columns]
                    if v < 3:
                        piece = piece + acc_ref[at + spots : at + spots + width, columns]
                    pieces.append(piece)
                stacked += exchange(pieces, count)
            flipped = jnp.concatenate(stacked, axis=0).T
            for v in range(first, first + per):
                send_ref[v * blocks + b] = flipped[(v - first) * count : (v - first + 1) * count]


def lagrange(coord, nodes_ref):
    weight = nodes_ref[0:8, :]
    spread_coord = jnp.broadcast_to(coord, (8, LANES))
    for k in range(1, 8):
        weight = weight * (spread_coord - nodes_ref[8 * k : 8 * k + 8, :])
    return weight


def interpolate(blocks, block, sources, recv_ref, fields_ref, nodes_ref, values_ref, picker_ref):
    near = fields_ref.shape[1] // 8
    nodes = fields_ref.shape[0] // 2
    zero = jnp.zeros((), BF16)
    ids = iota_bf16((near, LANES))
    weights = []
    for j, source in enumerate(sources):
        r, s, t, slot = [recv_ref[v * blocks + block, pl.ds(source, 1), :] for v in range(4)]
        weight_t = lagrange(t, nodes_ref)
        columns = slice(j * LANES, (j + 1) * LANES)
        far = jnp.broadcast_to(slot, (8, LANES)) >= float(near)
        mask = ids == spread(jnp.where(far[0:1], slot - float(near), slot), near)
        for c in range(8):
            picker_ref[c * near : (c + 1) * near, columns] = jnp.where(mask, spread(weight_t[c : c + 1, :], near), zero)
        weights.append((lagrange(r, nodes_ref), lagrange(s, nodes_ref), far))
    along = jnp.dot(fields_ref[...], picker_ref[...], preferred_element_type=F32)
    for j, source in enumerate(sources):
        weight_r, weight_s, far = weights[j]
        columns = slice(j * LANES, (j + 1) * LANES)
        factors = [jnp.broadcast_to(weight_r[a : a + 1, :], (8, LANES)) for a in range(8)]
        for f in range(4):
            total = None
            for a in range(8):
                at = f * 64 + a * 8
                here = jnp.where(far, along[nodes + at : nodes + at + 8, columns], along[at : at + 8, columns])
                total = here * factors[a] if a == 0 else total + here * factors[a]
            values_ref[f * blocks + block, pl.ds(source, 1), :] = jnp.sum(
                total * weight_s, axis=0, keepdims=True
            )


def sample_kernel(
    sizes,
    blocks,
    rank_in,
    coords_in,
    slot_in,
    fields_in,
    back_ref,
    row_ref,
    lane_ref,
    rank_ref,
    coords_ref,
    slot_ref,
    fields_ref,
    prefix_ref,
    nodes_ref,
    turned_ref,
    flip_ref,
    acc_ref,
    send_ref,
    recv_ref,
    values_ref,
    picker_even,
    picker_odd,
    out_sem,
    in_sem,
    back_out_sem,
    back_in_sem,
    own_sem,
    load_sem,
):
    count = sizes[0] * sizes[1] * sizes[2]
    place = [lax.axis_index(axis) for axis in AXES]
    me = (place[0] * sizes[1] + place[1]) * sizes[2] + place[2]
    mesh_ids = pl.DeviceIdType.MESH

    def peer(step, sign):
        offsets = [step // (sizes[1] * sizes[2]), step // sizes[2] % sizes[1], step % sizes[2]]
        at = tuple(lax.rem(p + n + sign * o, n) for p, n, o in zip(place, sizes, offsets))
        return (at[0] * sizes[1] + at[1]) * sizes[2] + at[2], at

    def each(first, last, act):
        def body(step, _):
            act(step)
            return 0

        lax.fori_loop(first, last, body, 0)

    def outward(step):
        other, at = peer(step, 1)
        return pltpu.make_async_remote_copy(
            src_ref=send_ref.at[:, other],
            dst_ref=recv_ref.at[:, me],
            send_sem=out_sem.at[step],
            recv_sem=in_sem.at[step],
            device_id=at,
            device_id_type=mesh_ids,
        )

    def backward(step):
        other, at = peer(step, -1)
        return pltpu.make_async_remote_copy(
            src_ref=values_ref.at[:, other],
            dst_ref=back_ref.at[:, me],
            send_sem=back_out_sem.at[step],
            recv_sem=back_in_sem.at[step],
            device_id=at,
            device_id_type=mesh_ids,
        )

    loads = [
        pltpu.make_async_copy(source, target, load_sem.at[i])
        for i, (source, target) in enumerate(
            [(rank_in, rank_ref), (coords_in, coords_ref), (slot_in, slot_ref), (fields_in, fields_ref)]
        )
    ]
    for load in loads:
        load.start()
    barrier = pltpu.get_barrier_semaphore()
    for step in range(1, count):
        pl.semaphore_signal(barrier, inc=1, device_id=peer(step, 1)[1], device_id_type=mesh_ids)
    prepare(prefix_ref, nodes_ref)
    loads[0].wait()
    place_all(count, rank_ref, prefix_ref, row_ref, lane_ref)
    for load in loads[1:]:
        load.wait()
    route(count, blocks, coords_ref, slot_ref, fields_ref, turned_ref, flip_ref, send_ref, row_ref, lane_ref, acc_ref)
    pl.semaphore_wait(barrier, count - 1)
    for step in range(1, count):
        outward(step).start()
    own = pltpu.make_async_copy(send_ref.at[:, me], recv_ref.at[:, me], own_sem.at[0])
    own.start()
    own.wait()
    own_back = pltpu.make_async_copy(values_ref.at[:, me], back_ref.at[:, me], own_sem.at[1])
    pickers = [picker_even, picker_odd]

    def reply(group):
        for j in range(GROUP):
            step = group * GROUP + j
            if j == 0:

                @pl.when(step == 0)
                def _():
                    own_back.start()

                @pl.when(step > 0)
                def _():
                    backward(step).start()

            else:
                backward(step).start()

    def body(group, _):
        @pl.when(group > 0)
        def _():
            reply(group - 1)

        sources = []
        for j in range(GROUP):
            step = group * GROUP + j
            if j == 0:

                @pl.when(step > 0)
                def _():
                    outward(step).wait_recv()

            else:
                outward(step).wait_recv()
            sources.append(peer(step, -1)[0])
        for block in range(blocks):
            interpolate(blocks, block, sources, recv_ref, turned_ref, nodes_ref, values_ref, pickers[block % 2])
        return 0

    groups = count // GROUP
    lax.fori_loop(0, groups, body, 0)
    reply(groups - 1)
    each(1, count, lambda step: outward(step).wait_send())
    each(1, count, lambda step: backward(step).wait())
    own_back.wait()


def return_kernel(blocks, values_ref, row_ref, lane_ref, out_ref, table_ref):
    probes = row_ref.shape[1]
    count = values_ref.shape[1]
    groups, width, per = splits(count)
    rows = groups * count
    spots = blocks * width
    for b in range(blocks):
        for first in range(0, 4, per):
            stacked = [values_ref[f * blocks + b] for f in range(first, first + per)]
            flipped = jnp.concatenate(stacked, axis=0).T
            for half in range(groups // per):
                pieces = [flipped[(half * per + q) * width : (half * per + q + 1) * width] for q in range(per)]
                for f, piece in enumerate(exchange(pieces, count), first):
                    at = f * spots + b * width
                    table_ref[at : at + width, half * LANES : (half + 1) * LANES] = piece.astype(BF16)
    row_ids = iota_bf16((rows, CHUNK))
    lane_ids = lax.broadcasted_iota(jnp.int32, (spots, CHUNK), 0).astype(F32)

    def body(step, _):
        for g in range(SWEEP):
            at = pl.ds(pl.multiple_of((step * SWEEP + g) * CHUNK, CHUNK), CHUNK)
            hot = jnp.where(row_ids == spread(row_ref[:, at], rows), jnp.ones((), BF16), jnp.zeros((), BF16))
            picked = jnp.dot(table_ref[...], hot, preferred_element_type=F32)
            here = lane_ids == jnp.broadcast_to(lane_ref[:, at], (spots, CHUNK))
            for f in range(4):
                out_ref[f : f + 1, at] = jnp.sum(
                    jnp.where(here, picked[f * spots : (f + 1) * spots], 0.0), axis=0, keepdims=True
                )
        return 0

    lax.fori_loop(0, probes // (SWEEP * CHUNK), body, 0)


VMEM = pl.BlockSpec(memory_space=pltpu.VMEM)
HBM = pl.BlockSpec(memory_space=pltpu.HBM)


def call(kernel, inputs, outputs, scratch, **options):
    return pl.pallas_call(
        kernel,
        out_shape=outputs,
        in_specs=inputs,
        out_specs=jax.tree.map(lambda _: VMEM, outputs),
        scratch_shapes=scratch,
        compiler_params=pltpu.CompilerParams(vmem_limit_bytes=48 << 20, **options),
    )


def local(sizes, fields, coordinates, element_rank, element_slot):
    count = sizes[0] * sizes[1] * sizes[2]
    probes = element_slot.shape[0]
    elements = fields.shape[0]
    capacity = 5 * probes // (4 * count)
    blocks = -(-capacity // LANES)
    layout = jax.ShapeDtypeStruct((4 * blocks, count, LANES), F32)
    line = jax.ShapeDtypeStruct((1, probes), F32)

    groups, width, _ = splits(count)
    spots, rows = blocks * width, groups * count
    depth = fields.shape[1] // 8
    picker = pltpu.VMEM((4 * elements, GROUP * LANES), BF16)
    buffer = pltpu.VMEM(layout.shape, F32)
    arrivals = pltpu.SemaphoreType.DMA((count,))
    returned, row, lane = call(
        functools.partial(sample_kernel, sizes, blocks),
        [HBM] * 4,
        (layout, line, line),
        [
            pltpu.VMEM((1, probes), jnp.int32),
            pltpu.VMEM((3, probes), F32),
            pltpu.VMEM((1, probes), jnp.int32),
            pltpu.VMEM(fields.shape, BF16),
            pltpu.VMEM((CHUNK, 2 * CHUNK), BF16),
            pltpu.VMEM((64, LANES), F32),
            pltpu.VMEM((2 * depth, 4 * elements), BF16),
            pltpu.VMEM((LANES, elements), F32),
            pltpu.VMEM((7 * spots, rows), F32),
        ]
        + [buffer] * 3
        + [picker] * 2
        + [arrivals] * 4
        + [pltpu.SemaphoreType.DMA((2,)), pltpu.SemaphoreType.DMA((4,))],
        collective_id=0,
        has_side_effects=True,
    )(
        *[
            pltpu.with_memory_space_constraint(x, pltpu.HBM)
            for x in (element_rank.reshape(1, probes), coordinates, element_slot.reshape(1, probes), fields)
        ]
    )
    return call(
        functools.partial(return_kernel, blocks),
        [VMEM] * 3,
        jax.ShapeDtypeStruct((4, probes), F32),
        [pltpu.VMEM((4 * spots, rows), BF16)],
    )(returned, row, lane)


def solution(mesh):
    sizes = tuple(mesh.shape[axis] for axis in AXES)
    placed = (P(AXES, None), P(None, AXES), P(AXES, None), P(AXES))
    return jax.shard_map(
        functools.partial(local, sizes),
        mesh=mesh,
        in_specs=placed,
        out_specs=P(None, AXES),
        check_vma=False,
    )
```

```python
import functools

import jax
import jax.numpy as jnp
import numpy as np
from jax import lax
from jax.experimental import pallas as pl
from jax.experimental.pallas import tpu as pltpu
from jax.sharding import PartitionSpec as P

AXES = ("gx", "gy", "gz")
F32, BF16 = jnp.float32, jnp.bfloat16
LANES = 128
CHUNK = 256
GROUP = 4
BATCH = 16
SWEEP = 32
SPAN = 1024.0

gll_points = np.array(
    [
        -1.0,
        -0.8717401485096066,
        -0.5917001814331423,
        -0.2092992179024789,
        0.2092992179024789,
        0.5917001814331423,
        0.8717401485096066,
        1.0,
    ]
)
gll_scale = np.array(
    [1.0 / np.prod([gll_points[a] - gll_points[b] for b in range(8) if b != a]) for a in range(8)]
)


def column(values):
    node = lax.broadcasted_iota(jnp.int32, (8, LANES), 0)
    out = jnp.full((8, LANES), float(values[0]), F32)
    for a in range(1, 8):
        out = jnp.where(node == a, float(values[a]), out)
    return out


def iota_bf16(shape):
    return lax.broadcasted_iota(jnp.int32, shape, 0).astype(F32).astype(BF16)


def spread(row, count):
    return jnp.broadcast_to(row, (count, row.shape[1])).astype(BF16)


def splits(count):
    groups = max(1, 2 * LANES // count)
    return groups, LANES // groups, max(1, LANES // count)


def exchange(pieces, count):
    block = lax.broadcasted_iota(jnp.int32, pieces[0].shape, 1) // count
    bit = len(pieces) // 2
    while bit:
        high = (block // bit) % 2 == 1
        swapped = []
        for i, own in enumerate(pieces):
            upper = (i // bit) % 2 == 1
            other = pltpu.roll(pieces[i - bit if upper else i + bit], LANES - bit * count if upper else bit * count, 1)
            swapped.append(jnp.where(high, own, other) if upper else jnp.where(high, other, own))
        pieces = swapped
        bit //= 2
    return pieces


def prepare(prefix_ref, nodes_ref):
    below = lax.broadcasted_iota(jnp.int32, (CHUNK, CHUNK), 0) <= lax.broadcasted_iota(jnp.int32, (CHUNK, CHUNK), 1)
    prefix_ref[:, :CHUNK] = jnp.where(below, 1.0, 0.0).astype(BF16)
    prefix_ref[:, CHUNK:] = jnp.ones((CHUNK, CHUNK), BF16)
    nodes_ref[0:8, :] = column(gll_scale)
    for k in range(1, 8):
        nodes_ref[8 * k : 8 * k + 8, :] = column(np.roll(gll_points, -k))


def turn(tile, fields_ref, turned_ref, flip_ref):
    elements = fields_ref.shape[0]
    columns = pl.ds(pl.multiple_of(tile * LANES, LANES), LANES)
    rows = pl.ds(pl.multiple_of(tile * 16, 16), 16)
    flip_ref[...] = fields_ref[:, columns].astype(F32).T
    near, nodes = elements // 2, turned_ref.shape[0] // 2
    beyond = pl.ds(pl.multiple_of(nodes + tile * 16, 16), 16)
    for c in range(0, 8, 2):
        one, two = [flip_ref[pl.ds(c + i, 16, stride=8), :] for i in range(2)]
        left = lax.broadcasted_iota(jnp.int32, one.shape, 1) < near
        turned_ref[rows, c * near : (c + 2) * near] = jnp.where(left, one, pltpu.roll(two, near, 1)).astype(BF16)
        turned_ref[beyond, c * near : (c + 2) * near] = jnp.where(left, pltpu.roll(one, near, 1), two).astype(BF16)


def offset_bits(sizes, group, j):
    rest = sizes[0] * sizes[1] * sizes[2] // (2 * GROUP)
    if isinstance(group, int):
        hot = int(1 <= group <= rest)
        which = group - 1 if hot else max(group - rest, 0)
    else:
        hot = (group + rest - 1) // rest % 2
        which = hot * (group - 1) + (1 - hot) * jnp.maximum(group - rest, 0)
    width = sum((n - 1).bit_length() for n in sizes)
    return [j % 2, j // 2 % 2, hot] + [which // 2**k % 2 for k in range(width - 3)]


def peer_of(sizes, place, group, j):
    bits = offset_bits(sizes, group, j)
    at = list(place)
    for axis in (2, 1, 0):
        for k in range((sizes[axis] - 1).bit_length()):
            at[axis] = at[axis] + bits.pop(0) * (1 - place[axis] // 2**k % 2 * 2) * 2**k
    return tuple(at)


def place_batch(count, step, targets, carry, rank_ref, prefix_ref, row_ref, lane_ref):
    group = min(BATCH, max(1, CHUNK // count))
    groups, width, _ = splits(count)
    for inner in range(BATCH // group):
        masks, hots = [], []
        places = [
            pl.ds(pl.multiple_of((step * BATCH + inner * group + g) * CHUNK, CHUNK), CHUNK) for g in range(group)
        ]
        for at in places:
            mask = targets == jnp.broadcast_to(rank_ref[:, at], (count, CHUNK))
            masks.append(mask)
            hots.append(jnp.where(mask, 1.0, 0.0).astype(BF16))
        counted = jnp.dot(jnp.concatenate(hots, axis=0), prefix_ref[...], preferred_element_type=F32)
        for g, at in enumerate(places):
            piece = counted[g * count : (g + 1) * count]
            place_in = jnp.where(masks[g], piece[:, :CHUNK] + carry, 0.0)
            found = jnp.sum(place_in, axis=0, keepdims=True) - 1.0
            peer = jnp.floor(found * (1.0 / SPAN))
            position = found - peer * SPAN
            part = jnp.floor(position * (1.0 / width))
            block = jnp.floor(part * (1.0 / groups))
            lane_ref[:, at] = position - (part - block) * width
            row_ref[:, at] = (part - block * groups) * count + peer
            carry = carry + piece[:, CHUNK:]
    return carry


def route(
    sizes,
    place,
    blocks,
    loads,
    rank_ref,
    coords_ref,
    slot_ref,
    fields_ref,
    prefix_ref,
    turned_ref,
    flip_ref,
    row_ref,
    lane_ref,
    acc_ref,
):
    count = sizes[0] * sizes[1] * sizes[2]
    probes = slot_ref.shape[1]
    groups, width, per = splits(count)
    rows = groups * count
    spots = blocks * width
    tiles = fields_ref.shape[1] // LANES
    steps = probes // (BATCH * CHUNK)
    steps_of = lax.broadcasted_iota(jnp.int32, (count, CHUNK), 0)
    x, y, z = peer_of(sizes, place, steps_of // GROUP, steps_of % GROUP)
    targets = (x * sizes[1] + y) * sizes[2] + z
    row_ids = iota_bf16((rows, CHUNK))
    lane_ids = iota_bf16((spots, CHUNK))
    one, zero = jnp.ones((), BF16), jnp.zeros((), BF16)
    acc_ref[...] = jnp.zeros_like(acc_ref)

    def put(step, carry):
        return place_batch(count, step, targets, carry, rank_ref, prefix_ref, row_ref, lane_ref)

    def scatter(step):
        row_hots, lane_parts = [], []
        for g in range(BATCH):
            at = pl.ds(pl.multiple_of((step * BATCH + g) * CHUNK, CHUNK), CHUNK)
            row_hots.append(jnp.where(row_ids == spread(row_ref[:, at], rows), one, zero))
            here = lane_ids == spread(lane_ref[:, at], spots)
            parts = []
            for v in range(3):
                value = coords_ref[v : v + 1, at]
                high = value.astype(BF16).astype(F32)
                parts += [high, value - high]
            parts.append(slot_ref[:, at].astype(F32))
            lane_parts.append(jnp.concatenate([jnp.where(here, spread(part, spots), zero) for part in parts], axis=0))
        acc_ref[...] += lax.dot_general(
            jnp.concatenate(lane_parts, axis=1),
            jnp.concatenate(row_hots, axis=1),
            (((1,), (1,)), ((), ())),
            preferred_element_type=F32,
        )
        for tile in range(tiles // steps):
            turn(step * (tiles // steps) + tile, fields_ref, turned_ref, flip_ref)

    def both(step, carry):
        scatter(step)
        return put(step + 1, carry)

    rank_ref[:, probes:] = jnp.zeros((1, rank_ref.shape[1] - probes), jnp.int32)
    loads[0].wait()
    carry = put(0, steps_of.astype(F32) * SPAN)
    for load in loads[1:]:
        load.wait()
    lax.fori_loop(0, steps, both, carry)


def assemble(count, blocks, acc_ref, send_ref, recv_ref):
    groups, width, per = splits(count)
    spots = blocks * width
    for b in range(blocks):
        for first in range(0, 4, per):
            stacked = []
            for half in range(groups // per):
                columns = slice(half * LANES, (half + 1) * LANES)
                pieces = []
                for v in range(first, first + per):
                    at = 2 * v * spots + b * width
                    piece = acc_ref[at : at + width, columns]
                    if v < 3:
                        piece = piece + acc_ref[at + spots : at + spots + width, columns]
                    pieces.append(piece)
                stacked += exchange(pieces, count)
            flipped = jnp.concatenate(stacked, axis=0).T
            for v in range(first, first + per):
                send_ref[v * blocks + b] = flipped[(v - first) * count : (v - first + 1) * count]
                recv_ref[v * blocks + b, 0:1] = flipped[(v - first) * count : (v - first) * count + 1]


def lagrange(coord, nodes_ref):
    weight = nodes_ref[0:8, :]
    spread_coord = jnp.broadcast_to(coord, (8, LANES))
    for k in range(1, 8):
        weight = weight * (spread_coord - nodes_ref[8 * k : 8 * k + 8, :])
    return weight


def pick(blocks, block, first, recv_ref, nodes_ref, picker_ref):
    near = picker_ref.shape[0] // 8
    zero = jnp.zeros((), BF16)
    ids = iota_bf16((near, LANES))
    for j in range(GROUP):
        t, slot = [recv_ref[v * blocks + block, pl.ds(first + j, 1), :] for v in (2, 3)]
        weight_t = lagrange(t, nodes_ref)
        columns = slice(j * LANES, (j + 1) * LANES)
        mask = ids == spread(jnp.where(slot >= float(near), slot - float(near), slot), near)
        for c in range(8):
            picker_ref[c * near : (c + 1) * near, columns] = jnp.where(mask, spread(weight_t[c : c + 1, :], near), zero)


def combine(blocks, block, first, recv_ref, fields_ref, nodes_ref, values_ref, picker_ref):
    near = picker_ref.shape[0] // 8
    nodes = fields_ref.shape[0] // 2
    along = jnp.dot(fields_ref[...], picker_ref[...], preferred_element_type=F32)
    for j in range(GROUP):
        r, s, slot = [recv_ref[v * blocks + block, pl.ds(first + j, 1), :] for v in (0, 1, 3)]
        weight_r, weight_s = lagrange(r, nodes_ref), lagrange(s, nodes_ref)
        far = jnp.broadcast_to(slot, (8, LANES)) >= float(near)
        columns = slice(j * LANES, (j + 1) * LANES)
        factors = [jnp.broadcast_to(weight_r[a : a + 1, :], (8, LANES)) for a in range(8)]
        for f in range(4):
            total = None
            for a in range(8):
                at = f * 64 + a * 8
                here = jnp.where(far, along[nodes + at : nodes + at + 8, columns], along[at : at + 8, columns])
                total = here * factors[a] if a == 0 else total + here * factors[a]
            values_ref[f * blocks + block, pl.ds(first + j, 1), :] = jnp.sum(
                total * weight_s, axis=0, keepdims=True
            )


def sample_kernel(
    sizes,
    blocks,
    rank_in,
    coords_in,
    slot_in,
    fields_in,
    back_ref,
    row_ref,
    lane_ref,
    rank_ref,
    coords_ref,
    slot_ref,
    fields_ref,
    prefix_ref,
    nodes_ref,
    turned_ref,
    flip_ref,
    acc_ref,
    send_ref,
    recv_ref,
    values_ref,
    picker_even,
    picker_odd,
    out_sem,
    in_sem,
    back_out_sem,
    back_in_sem,
    load_sem,
):
    count = sizes[0] * sizes[1] * sizes[2]
    place = [lax.axis_index(axis) for axis in AXES]
    mesh_ids = pl.DeviceIdType.MESH

    def each(first, last, act):
        def body(step, _):
            act(step)
            return 0

        lax.fori_loop(first, last, body, 0)

    def outward(group, j):
        step = group * GROUP + j
        return pltpu.make_async_remote_copy(
            src_ref=send_ref.at[:, step],
            dst_ref=recv_ref.at[:, step],
            send_sem=out_sem.at[step],
            recv_sem=in_sem.at[step],
            device_id=peer_of(sizes, place, group, j),
            device_id_type=mesh_ids,
        )

    def backward(group, j):
        step = group * GROUP + j
        return pltpu.make_async_remote_copy(
            src_ref=values_ref.at[:, step],
            dst_ref=back_ref.at[:, step],
            send_sem=back_out_sem.at[step],
            recv_sem=back_in_sem.at[step],
            device_id=peer_of(sizes, place, group, j),
            device_id_type=mesh_ids,
        )

    loads = [
        pltpu.make_async_copy(source, target, load_sem.at[i])
        for i, (source, target) in enumerate(
            [(rank_in, rank_ref.at[:, : rank_in.shape[1]]), (coords_in, coords_ref), (slot_in, slot_ref), (fields_in, fields_ref)]
        )
    ]
    for load in loads:
        load.start()
    barrier = pltpu.get_barrier_semaphore()
    others = [(group, j) for group in range(count // GROUP) for j in range(GROUP) if group or j]
    for group, j in others:
        pl.semaphore_signal(barrier, inc=1, device_id=peer_of(sizes, place, group, j), device_id_type=mesh_ids)
    prepare(prefix_ref, nodes_ref)
    route(
        sizes,
        place,
        blocks,
        loads,
        rank_ref,
        coords_ref,
        slot_ref,
        fields_ref,
        prefix_ref,
        turned_ref,
        flip_ref,
        row_ref,
        lane_ref,
        acc_ref,
    )
    pl.semaphore_wait(barrier, count - 1)
    assemble(count, blocks, acc_ref, send_ref, recv_ref)
    for group, j in others:
        outward(group, j).start()
    groups = count // GROUP
    pickers = [picker_even, picker_odd]

    def reply(group, skip):
        for j in range(skip, GROUP):
            backward(group, j).start()

    def serve(group):
        first = group * GROUP
        for block in range(blocks):
            pick(blocks, block, first, recv_ref, nodes_ref, pickers[block % 2])
            combine(blocks, block, first, recv_ref, turned_ref, nodes_ref, values_ref, pickers[block % 2])

    def body(group, _):
        @pl.when(group > 1)
        def _():
            backward(group - 1, 0).start()

        @pl.when(group > 0)
        def _():
            reply(group - 1, 1)
            outward(group, 0).wait_recv()

        for j in range(1, GROUP):
            outward(group, j).wait_recv()
        serve(group)
        return 0

    lax.fori_loop(0, groups, body, 0)
    reply(groups - 1, 0)
    back_ref[:, 0:1] = values_ref[:, 0:1]

    def finish(group, skip):
        for j in range(skip, GROUP):
            outward(group, j).wait_send()
            backward(group, j).wait()

    def rest(group, _):
        finish(group, 0)
        return 0

    finish(0, 1)
    lax.fori_loop(1, groups, rest, 0)


def return_kernel(blocks, values_ref, row_ref, lane_ref, out_ref, table_ref):
    probes = out_ref.shape[1]
    count = values_ref.shape[1]
    groups, width, per = splits(count)
    rows = groups * count
    spots = blocks * width
    for b in range(blocks):
        for first in range(0, 4, per):
            stacked = [values_ref[f * blocks + b] for f in range(first, first + per)]
            flipped = jnp.concatenate(stacked, axis=0).T
            for half in range(groups // per):
                pieces = [flipped[(half * per + q) * width : (half * per + q + 1) * width] for q in range(per)]
                for f, piece in enumerate(exchange(pieces, count), first):
                    at = f * spots + b * width
                    table_ref[at : at + width, half * LANES : (half + 1) * LANES] = piece.astype(BF16)
    row_ids = iota_bf16((rows, CHUNK))
    lane_ids = lax.broadcasted_iota(jnp.int32, (spots, CHUNK), 0).astype(F32)

    def body(step, _):
        for g in range(SWEEP):
            at = pl.ds(pl.multiple_of((step * SWEEP + g) * CHUNK, CHUNK), CHUNK)
            hot = jnp.where(row_ids == spread(row_ref[:, at], rows), jnp.ones((), BF16), jnp.zeros((), BF16))
            picked = jnp.dot(table_ref[...], hot, preferred_element_type=F32)
            here = lane_ids == jnp.broadcast_to(lane_ref[:, at], (spots, CHUNK))
            for f in range(4):
                out_ref[f : f + 1, at] = jnp.sum(
                    jnp.where(here, picked[f * spots : (f + 1) * spots], 0.0), axis=0, keepdims=True
                )
        return 0

    lax.fori_loop(0, probes // (SWEEP * CHUNK), body, 0)


VMEM = pl.BlockSpec(memory_space=pltpu.VMEM)
HBM = pl.BlockSpec(memory_space=pltpu.HBM)


def call(kernel, inputs, outputs, scratch, **options):
    return pl.pallas_call(
        kernel,
        out_shape=outputs,
        in_specs=inputs,
        out_specs=jax.tree.map(lambda _: VMEM, outputs),
        scratch_shapes=scratch,
        compiler_params=pltpu.CompilerParams(vmem_limit_bytes=48 << 20, **options),
    )


def local(sizes, fields, coordinates, element_rank, element_slot):
    count = sizes[0] * sizes[1] * sizes[2]
    probes = element_slot.shape[0]
    elements = fields.shape[0]
    capacity = 5 * probes // (4 * count)
    blocks = -(-capacity // LANES)
    layout = jax.ShapeDtypeStruct((4 * blocks, count, LANES), F32)
    line = jax.ShapeDtypeStruct((1, probes + BATCH * CHUNK), F32)

    groups, width, _ = splits(count)
    spots, rows = blocks * width, groups * count
    depth = fields.shape[1] // 8
    picker = pltpu.VMEM((4 * elements, GROUP * LANES), BF16)
    buffer = pltpu.VMEM(layout.shape, F32)
    arrivals = pltpu.SemaphoreType.DMA((count,))
    returned, row, lane = call(
        functools.partial(sample_kernel, sizes, blocks),
        [HBM] * 4,
        (layout, line, line),
        [
            pltpu.VMEM(line.shape, jnp.int32),
            pltpu.VMEM((3, probes), F32),
            pltpu.VMEM((1, probes), jnp.int32),
            pltpu.VMEM(fields.shape, BF16),
            pltpu.VMEM((CHUNK, 2 * CHUNK), BF16),
            pltpu.VMEM((64, LANES), F32),
            pltpu.VMEM((2 * depth, 4 * elements), BF16),
            pltpu.VMEM((LANES, elements), F32),
            pltpu.VMEM((7 * spots, rows), F32),
        ]
        + [buffer] * 3
        + [picker] * 2
        + [arrivals] * 4
        + [pltpu.SemaphoreType.DMA((4,))],
        collective_id=0,
        has_side_effects=True,
    )(
        *[
            pltpu.with_memory_space_constraint(x, pltpu.HBM)
            for x in (element_rank.reshape(1, probes), coordinates, element_slot.reshape(1, probes), fields)
        ]
    )
    return call(
        functools.partial(return_kernel, blocks),
        [VMEM] * 3,
        jax.ShapeDtypeStruct((4, probes), F32),
        [pltpu.VMEM((4 * spots, rows), BF16)],
    )(returned, row, lane)


def solution(mesh):
    sizes = tuple(mesh.shape[axis] for axis in AXES)
    placed = (P(AXES, None), P(None, AXES), P(AXES, None), P(AXES))
    return jax.shard_map(
        functools.partial(local, sizes),
        mesh=mesh,
        in_specs=placed,
        out_specs=P(None, AXES),
        check_vma=False,
    )
```

```python
import functools

import jax
import jax.numpy as jnp
import numpy as np
from jax import lax
from jax.experimental import pallas as pl
from jax.experimental.pallas import tpu as pltpu
from jax.sharding import PartitionSpec as P

AXES = ("gx", "gy", "gz")
F32, BF16 = jnp.float32, jnp.bfloat16
LANES = 128
CHUNK = 256
GROUP = 4
BATCH = 16
SWEEP = 32
SPAN = 1024.0
COARSE = 256.0
FINE = 64.0
LEAD = 1

gll_points = np.array(
    [
        -1.0,
        -0.8717401485096066,
        -0.5917001814331423,
        -0.2092992179024789,
        0.2092992179024789,
        0.5917001814331423,
        0.8717401485096066,
        1.0,
    ]
)
gll_scale = np.array(
    [1.0 / np.prod([gll_points[a] - gll_points[b] for b in range(8) if b != a]) for a in range(8)]
)


def column(values):
    node = lax.broadcasted_iota(jnp.int32, (8, LANES), 0)
    out = jnp.full((8, LANES), float(values[0]), F32)
    for a in range(1, 8):
        out = jnp.where(node == a, float(values[a]), out)
    return out


def iota_bf16(shape):
    return lax.broadcasted_iota(jnp.int32, shape, 0).astype(F32).astype(BF16)


def spread(row, count):
    return jnp.broadcast_to(row, (count, row.shape[1])).astype(BF16)


def splits(count):
    groups = max(1, 2 * LANES // count)
    return groups, LANES // groups, max(1, LANES // count)


def exchange(pieces, count):
    block = lax.broadcasted_iota(jnp.int32, pieces[0].shape, 1) // count
    bit = len(pieces) // 2
    while bit:
        high = (block // bit) % 2 == 1
        swapped = []
        for i, own in enumerate(pieces):
            upper = (i // bit) % 2 == 1
            other = pltpu.roll(pieces[i - bit if upper else i + bit], LANES - bit * count if upper else bit * count, 1)
            swapped.append(jnp.where(high, own, other) if upper else jnp.where(high, other, own))
        pieces = swapped
        bit //= 2
    return pieces


def prepare(prefix_ref, nodes_ref):
    below = lax.broadcasted_iota(jnp.int32, (CHUNK, CHUNK), 0) <= lax.broadcasted_iota(jnp.int32, (CHUNK, CHUNK), 1)
    prefix_ref[:, :CHUNK] = jnp.where(below, 1.0, 0.0).astype(BF16)
    prefix_ref[:, CHUNK:] = jnp.ones((CHUNK, CHUNK), BF16)
    nodes_ref[0:8, :] = column(gll_scale)
    for k in range(1, 8):
        nodes_ref[8 * k : 8 * k + 8, :] = column(np.roll(gll_points, -k))


def turn(tile, fields_ref, turned_ref, flip_ref):
    elements = fields_ref.shape[0]
    columns = pl.ds(pl.multiple_of(tile * LANES, LANES), LANES)
    rows = pl.ds(pl.multiple_of(tile * 16, 16), 16)
    flip_ref[...] = fields_ref[:, columns].astype(F32).T
    near, nodes = elements // 2, turned_ref.shape[0] // 2
    beyond = pl.ds(pl.multiple_of(nodes + tile * 16, 16), 16)
    for c in range(0, 8, 2):
        one, two = [flip_ref[pl.ds(c + i, 16, stride=8), :] for i in range(2)]
        left = lax.broadcasted_iota(jnp.int32, one.shape, 1) < near
        turned_ref[rows, c * near : (c + 2) * near] = jnp.where(left, one, pltpu.roll(two, near, 1)).astype(BF16)
        turned_ref[beyond, c * near : (c + 2) * near] = jnp.where(left, pltpu.roll(one, near, 1), two).astype(BF16)


def offset_bits(sizes, group, j):
    rest = sizes[0] * sizes[1] * sizes[2] // (2 * GROUP)
    hot = (group + rest - LEAD - 1) // rest % 2
    if isinstance(group, int):
        cold = min(group, max(group - rest, LEAD))
    else:
        cold = jnp.minimum(group, jnp.maximum(group - rest, LEAD))
    which = hot * (group - LEAD - 1) + (1 - hot) * cold
    width = sum((n - 1).bit_length() for n in sizes)
    return [j % 2, j // 2 % 2, hot] + [which // 2**k % 2 for k in range(width - 3)]


def peer_of(sizes, place, group, j):
    bits = offset_bits(sizes, group, j)
    at = list(place)
    for axis in (2, 1, 0):
        for k in range((sizes[axis] - 1).bit_length()):
            at[axis] = at[axis] + bits.pop(0) * (1 - place[axis] // 2**k % 2 * 2) * 2**k
    return tuple(at)


def place_batch(count, step, targets, carry, rank_ref, prefix_ref, row_ref, lane_ref):
    group = min(BATCH, max(1, CHUNK // count))
    groups, width, _ = splits(count)
    for inner in range(BATCH // group):
        masks, hots = [], []
        places = [
            pl.ds(pl.multiple_of((step * BATCH + inner * group + g) * CHUNK, CHUNK), CHUNK) for g in range(group)
        ]
        for at in places:
            mask = targets == jnp.broadcast_to(rank_ref[:, at], (count, CHUNK))
            masks.append(mask)
            hots.append(jnp.where(mask, 1.0, 0.0).astype(BF16))
        counted = jnp.dot(jnp.concatenate(hots, axis=0), prefix_ref[...], preferred_element_type=F32)
        for g, at in enumerate(places):
            piece = counted[g * count : (g + 1) * count]
            place_in = jnp.where(masks[g], piece[:, :CHUNK] + carry, 0.0)
            found = jnp.sum(place_in, axis=0, keepdims=True) - 1.0
            peer = jnp.floor(found * (1.0 / SPAN))
            position = found - peer * SPAN
            part = jnp.floor(position * (1.0 / width))
            block = jnp.floor(part * (1.0 / groups))
            lane_ref[:, at] = position - (part - block) * width
            row_ref[:, at] = (part - block * groups) * count + peer
            carry = carry + piece[:, CHUNK:]
    return carry


def route(
    sizes,
    place,
    blocks,
    loads,
    rank_ref,
    coords_ref,
    slot_ref,
    fields_ref,
    prefix_ref,
    turned_ref,
    flip_ref,
    row_ref,
    lane_ref,
    acc_ref,
):
    count = sizes[0] * sizes[1] * sizes[2]
    probes = slot_ref.shape[1]
    groups, width, per = splits(count)
    rows = groups * count
    spots = blocks * width
    tiles = fields_ref.shape[1] // LANES
    steps = probes // (BATCH * CHUNK)
    steps_of = lax.broadcasted_iota(jnp.int32, (count, CHUNK), 0)
    x, y, z = peer_of(sizes, place, steps_of // GROUP, steps_of % GROUP)
    targets = (x * sizes[1] + y) * sizes[2] + z
    row_ids = iota_bf16((rows, CHUNK))
    lane_ids = iota_bf16((spots, CHUNK))
    one, zero = jnp.ones((), BF16), jnp.zeros((), BF16)
    acc_ref[...] = jnp.zeros_like(acc_ref)

    def put(step, carry):
        return place_batch(count, step, targets, carry, rank_ref, prefix_ref, row_ref, lane_ref)

    def scatter(step):
        row_hots, lane_parts = [], []
        for g in range(BATCH):
            at = pl.ds(pl.multiple_of((step * BATCH + g) * CHUNK, CHUNK), CHUNK)
            row_hots.append(jnp.where(row_ids == spread(row_ref[:, at], rows), one, zero))
            here = lane_ids == spread(lane_ref[:, at], spots)
            parts = []
            slot = slot_ref[:, at]
            digits = [slot & 7, (slot >> 3) & 7, slot >> 6]
            for v in range(3):
                value = coords_ref[v : v + 1, at] * COARSE
                high = jnp.floor(value)
                low = jnp.floor((value - high) * FINE)
                parts += [high, low + (digits[v] * int(FINE) - int(COARSE)).astype(F32)]
            lane_parts.append(jnp.concatenate([jnp.where(here, spread(part, spots), zero) for part in parts], axis=0))
        acc_ref[...] += lax.dot_general(
            jnp.concatenate(lane_parts, axis=1),
            jnp.concatenate(row_hots, axis=1),
            (((1,), (1,)), ((), ())),
            preferred_element_type=F32,
        )
        for tile in range(tiles // steps):
            turn(step * (tiles // steps) + tile, fields_ref, turned_ref, flip_ref)

    def both(step, carry):
        scatter(step)
        return put(step + 1, carry)

    rank_ref[:, probes:] = jnp.zeros((1, rank_ref.shape[1] - probes), jnp.int32)
    loads[0].wait()
    carry = put(0, steps_of.astype(F32) * SPAN)
    for load in loads[1:]:
        load.wait()
    lax.fori_loop(0, steps, both, carry)


def assemble(count, blocks, acc_ref, send_ref, recv_ref):
    groups, width, per = splits(count)
    spots = blocks * width
    for b in range(blocks):
        for first in range(0, 4, per):
            stacked = []
            for half in range(groups // per):
                columns = slice(half * LANES, (half + 1) * LANES)
                values, slot = [], 0.0
                for v in range(3):
                    at = 2 * v * spots + b * width
                    high = acc_ref[at : at + width, columns]
                    low = acc_ref[at + spots : at + spots + width, columns] + COARSE
                    digit = jnp.floor(low * (1.0 / FINE))
                    values.append((high + (low - digit * FINE + 0.5) * (1.0 / FINE)) * (1.0 / COARSE))
                    slot = slot + digit * float(8**v)
                values.append(slot)
                pieces = values[first : first + per]
                stacked += exchange(pieces, count)
            flipped = jnp.concatenate(stacked, axis=0).T
            for v in range(first, first + per):
                send_ref[v * blocks + b] = flipped[(v - first) * count : (v - first + 1) * count]
                recv_ref[v * blocks + b, 0:1] = flipped[(v - first) * count : (v - first) * count + 1]


def lagrange(coord, nodes_ref):
    weight = nodes_ref[0:8, :]
    spread_coord = jnp.broadcast_to(coord, (8, LANES))
    for k in range(1, 8):
        weight = weight * (spread_coord - nodes_ref[8 * k : 8 * k + 8, :])
    return weight


def pick(blocks, block, first, recv_ref, nodes_ref, picker_ref):
    near = picker_ref.shape[0] // 8
    zero = jnp.zeros((), BF16)
    ids = iota_bf16((near, LANES))
    for j in range(GROUP):
        t, slot = [recv_ref[v * blocks + block, pl.ds(first + j, 1), :] for v in (2, 3)]
        weight_t = lagrange(t, nodes_ref)
        columns = slice(j * LANES, (j + 1) * LANES)
        mask = ids == spread(jnp.where(slot >= float(near), slot - float(near), slot), near)
        for c in range(8):
            picker_ref[c * near : (c + 1) * near, columns] = jnp.where(mask, spread(weight_t[c : c + 1, :], near), zero)


def combine(blocks, block, first, recv_ref, fields_ref, nodes_ref, values_ref, picker_ref):
    near = picker_ref.shape[0] // 8
    nodes = fields_ref.shape[0] // 2
    along = jnp.dot(fields_ref[...], picker_ref[...], preferred_element_type=F32)
    for j in range(GROUP):
        r, s, slot = [recv_ref[v * blocks + block, pl.ds(first + j, 1), :] for v in (0, 1, 3)]
        weight_r, weight_s = lagrange(r, nodes_ref), lagrange(s, nodes_ref)
        far = jnp.broadcast_to(slot, (8, LANES)) >= float(near)
        columns = slice(j * LANES, (j + 1) * LANES)
        factors = [jnp.broadcast_to(weight_r[a : a + 1, :], (8, LANES)) for a in range(8)]
        for f in range(4):
            total = None
            for a in range(8):
                at = f * 64 + a * 8
                here = jnp.where(far, along[nodes + at : nodes + at + 8, columns], along[at : at + 8, columns])
                total = here * factors[a] if a == 0 else total + here * factors[a]
            values_ref[f * blocks + block, pl.ds(first + j, 1), :] = jnp.sum(
                total * weight_s, axis=0, keepdims=True
            )


def sample_kernel(
    sizes,
    blocks,
    rank_in,
    coords_in,
    slot_in,
    fields_in,
    back_ref,
    row_ref,
    lane_ref,
    rank_ref,
    coords_ref,
    slot_ref,
    fields_ref,
    prefix_ref,
    nodes_ref,
    turned_ref,
    flip_ref,
    acc_ref,
    send_ref,
    recv_ref,
    values_ref,
    picker_even,
    picker_odd,
    out_sem,
    in_sem,
    back_out_sem,
    back_in_sem,
    load_sem,
):
    count = sizes[0] * sizes[1] * sizes[2]
    place = [lax.axis_index(axis) for axis in AXES]
    mesh_ids = pl.DeviceIdType.MESH

    def each(first, last, act):
        def body(step, _):
            act(step)
            return 0

        lax.fori_loop(first, last, body, 0)

    def outward(group, j):
        step = group * GROUP + j
        return pltpu.make_async_remote_copy(
            src_ref=send_ref.at[:, step],
            dst_ref=recv_ref.at[:, step],
            send_sem=out_sem.at[step],
            recv_sem=in_sem.at[step],
            device_id=peer_of(sizes, place, group, j),
            device_id_type=mesh_ids,
        )

    def backward(group, j):
        step = group * GROUP + j
        return pltpu.make_async_remote_copy(
            src_ref=values_ref.at[:, step],
            dst_ref=back_ref.at[:, step],
            send_sem=back_out_sem.at[step],
            recv_sem=back_in_sem.at[step],
            device_id=peer_of(sizes, place, group, j),
            device_id_type=mesh_ids,
        )

    loads = [
        pltpu.make_async_copy(source, target, load_sem.at[i])
        for i, (source, target) in enumerate(
            [(rank_in, rank_ref.at[:, : rank_in.shape[1]]), (coords_in, coords_ref), (slot_in, slot_ref), (fields_in, fields_ref)]
        )
    ]
    for load in loads:
        load.start()
    barrier = pltpu.get_barrier_semaphore()
    others = [(group, j) for group in range(count // GROUP) for j in range(GROUP) if group or j]
    for group, j in others:
        pl.semaphore_signal(barrier, inc=1, device_id=peer_of(sizes, place, group, j), device_id_type=mesh_ids)
    prepare(prefix_ref, nodes_ref)
    route(
        sizes,
        place,
        blocks,
        loads,
        rank_ref,
        coords_ref,
        slot_ref,
        fields_ref,
        prefix_ref,
        turned_ref,
        flip_ref,
        row_ref,
        lane_ref,
        acc_ref,
    )
    pl.semaphore_wait(barrier, count - 1)
    assemble(count, blocks, acc_ref, send_ref, recv_ref)
    groups = count // GROUP
    early = [g for g in range(groups) if g == 0 or offset_bits(sizes, g, 0)[2]]
    for group, j in sorted(others, key=lambda at: at[0] not in early):
        outward(group, j).start()
    pickers = [picker_even, picker_odd]

    def serve(group):
        first = group * GROUP
        for block in range(blocks):
            pick(blocks, block, first, recv_ref, nodes_ref, pickers[block % 2])
            combine(blocks, block, first, recv_ref, turned_ref, nodes_ref, values_ref, pickers[block % 2])

    def body(group, _):
        @pl.when(group > 0)
        def _():
            outward(group, 0).wait_recv()

        for j in range(1, GROUP):
            outward(group, j).wait_recv()
        serve(group)
        for j in range(1, GROUP):
            backward(group, j).start()

        @pl.when(group > 0)
        def _():
            backward(group, 0).start()

        return 0

    lax.fori_loop(0, groups, body, 0)
    back_ref[:, 0:1] = values_ref[:, 0:1]

    def finish(group, skip):
        for j in range(skip, GROUP):
            outward(group, j).wait_send()
            backward(group, j).wait()

    def rest(group, _):
        finish(group, 0)
        return 0

    finish(0, 1)
    lax.fori_loop(1, groups, rest, 0)


def return_kernel(blocks, values_ref, row_ref, lane_ref, out_ref, table_ref):
    probes = out_ref.shape[1]
    count = values_ref.shape[1]
    groups, width, per = splits(count)
    rows = groups * count
    spots = blocks * width
    for b in range(blocks):
        for first in range(0, 4, per):
            stacked = [values_ref[f * blocks + b] for f in range(first, first + per)]
            flipped = jnp.concatenate(stacked, axis=0).T
            for half in range(groups // per):
                pieces = [flipped[(half * per + q) * width : (half * per + q + 1) * width] for q in range(per)]
                for f, piece in enumerate(exchange(pieces, count), first):
                    at = f * spots + b * width
                    table_ref[at : at + width, half * LANES : (half + 1) * LANES] = piece.astype(BF16)
    row_ids = iota_bf16((rows, CHUNK))
    lane_ids = lax.broadcasted_iota(jnp.int32, (spots, CHUNK), 0).astype(F32)

    def body(step, _):
        for g in range(SWEEP):
            at = pl.ds(pl.multiple_of((step * SWEEP + g) * CHUNK, CHUNK), CHUNK)
            hot = jnp.where(row_ids == spread(row_ref[:, at], rows), jnp.ones((), BF16), jnp.zeros((), BF16))
            picked = jnp.dot(table_ref[...], hot, preferred_element_type=F32)
            here = lane_ids == jnp.broadcast_to(lane_ref[:, at], (spots, CHUNK))
            for f in range(4):
                out_ref[f : f + 1, at] = jnp.sum(
                    jnp.where(here, picked[f * spots : (f + 1) * spots], 0.0), axis=0, keepdims=True
                )
        return 0

    lax.fori_loop(0, probes // (SWEEP * CHUNK), body, 0)


VMEM = pl.BlockSpec(memory_space=pltpu.VMEM)
HBM = pl.BlockSpec(memory_space=pltpu.HBM)


def call(kernel, inputs, outputs, scratch, **options):
    return pl.pallas_call(
        kernel,
        out_shape=outputs,
        in_specs=inputs,
        out_specs=jax.tree.map(lambda _: VMEM, outputs),
        scratch_shapes=scratch,
        compiler_params=pltpu.CompilerParams(vmem_limit_bytes=48 << 20, **options),
    )


def local(sizes, fields, coordinates, element_rank, element_slot):
    count = sizes[0] * sizes[1] * sizes[2]
    probes = element_slot.shape[0]
    elements = fields.shape[0]
    capacity = 5 * probes // (4 * count)
    blocks = -(-capacity // LANES)
    layout = jax.ShapeDtypeStruct((4 * blocks, count, LANES), F32)
    line = jax.ShapeDtypeStruct((1, probes + BATCH * CHUNK), F32)

    groups, width, _ = splits(count)
    spots, rows = blocks * width, groups * count
    depth = fields.shape[1] // 8
    picker = pltpu.VMEM((4 * elements, GROUP * LANES), BF16)
    buffer = pltpu.VMEM(layout.shape, F32)
    arrivals = pltpu.SemaphoreType.DMA((count,))
    returned, row, lane = call(
        functools.partial(sample_kernel, sizes, blocks),
        [HBM] * 4,
        (layout, line, line),
        [
            pltpu.VMEM(line.shape, jnp.int32),
            pltpu.VMEM((3, probes), F32),
            pltpu.VMEM((1, probes), jnp.int32),
            pltpu.VMEM(fields.shape, BF16),
            pltpu.VMEM((CHUNK, 2 * CHUNK), BF16),
            pltpu.VMEM((64, LANES), F32),
            pltpu.VMEM((2 * depth, 4 * elements), BF16),
            pltpu.VMEM((LANES, elements), F32),
            pltpu.VMEM((6 * spots, rows), F32),
        ]
        + [buffer] * 3
        + [picker] * 2
        + [arrivals] * 4
        + [pltpu.SemaphoreType.DMA((4,))],
        collective_id=0,
        has_side_effects=True,
    )(
        *[
            pltpu.with_memory_space_constraint(x, pltpu.HBM)
            for x in (element_rank.reshape(1, probes), coordinates, element_slot.reshape(1, probes), fields)
        ]
    )
    return call(
        functools.partial(return_kernel, blocks),
        [VMEM] * 3,
        jax.ShapeDtypeStruct((4, probes), F32),
        [pltpu.VMEM((4 * spots, rows), BF16)],
    )(returned, row, lane)


def solution(mesh):
    sizes = tuple(mesh.shape[axis] for axis in AXES)
    placed = (P(AXES, None), P(None, AXES), P(AXES, None), P(AXES))
    return jax.shard_map(
        functools.partial(local, sizes),
        mesh=mesh,
        in_specs=placed,
        out_specs=P(None, AXES),
        check_vma=False,
    )
```

```python
import functools

import jax
import jax.numpy as jnp
import numpy as np
from jax import lax
from jax.experimental import pallas as pl
from jax.experimental.pallas import tpu as pltpu
from jax.sharding import PartitionSpec as P

AXES = ("gx", "gy", "gz")
F32, BF16 = jnp.float32, jnp.bfloat16
LANES = 128
CHUNK = 256
GROUP = 4
BATCH = 16
SWEEP = 32
SPAN = 1024.0
COARSE = 256.0
FINE = 64.0

gll_points = np.array(
    [
        -1.0,
        -0.8717401485096066,
        -0.5917001814331423,
        -0.2092992179024789,
        0.2092992179024789,
        0.5917001814331423,
        0.8717401485096066,
        1.0,
    ]
)
gll_scale = np.array(
    [1.0 / np.prod([gll_points[a] - gll_points[b] for b in range(8) if b != a]) for a in range(8)]
)


def column(values):
    node = lax.broadcasted_iota(jnp.int32, (8, LANES), 0)
    out = jnp.full((8, LANES), float(values[0]), F32)
    for a in range(1, 8):
        out = jnp.where(node == a, float(values[a]), out)
    return out


def iota_bf16(shape):
    return lax.broadcasted_iota(jnp.int32, shape, 0).astype(F32).astype(BF16)


def spread(row, count):
    return jnp.broadcast_to(row, (count, row.shape[1])).astype(BF16)


def splits(count):
    groups = max(1, 2 * LANES // count)
    return groups, LANES // groups, max(1, LANES // count)


def exchange(pieces, count):
    block = lax.broadcasted_iota(jnp.int32, pieces[0].shape, 1) // count
    bit = len(pieces) // 2
    while bit:
        high = (block // bit) % 2 == 1
        swapped = []
        for i, own in enumerate(pieces):
            upper = (i // bit) % 2 == 1
            other = pltpu.roll(pieces[i - bit if upper else i + bit], LANES - bit * count if upper else bit * count, 1)
            swapped.append(jnp.where(high, own, other) if upper else jnp.where(high, other, own))
        pieces = swapped
        bit //= 2
    return pieces


def prepare(prefix_ref, nodes_ref):
    below = lax.broadcasted_iota(jnp.int32, (CHUNK, CHUNK), 0) <= lax.broadcasted_iota(jnp.int32, (CHUNK, CHUNK), 1)
    prefix_ref[:, :CHUNK] = jnp.where(below, 1.0, 0.0).astype(BF16)
    prefix_ref[:, CHUNK:] = jnp.ones((CHUNK, CHUNK), BF16)
    nodes_ref[0:8, :] = column(gll_scale)
    for k in range(1, 8):
        nodes_ref[8 * k : 8 * k + 8, :] = column(np.roll(gll_points, -k))


def turn(tile, fields_ref, turned_ref, flip_ref):
    elements = fields_ref.shape[0]
    columns = pl.ds(pl.multiple_of(tile * LANES, LANES), LANES)
    rows = pl.ds(pl.multiple_of(tile * 16, 16), 16)
    flip_ref[...] = fields_ref[:, columns].astype(F32).T
    near, nodes = elements // 2, turned_ref.shape[0] // 2
    beyond = pl.ds(pl.multiple_of(nodes + tile * 16, 16), 16)
    for c in range(0, 8, 2):
        one, two = [flip_ref[pl.ds(c + i, 16, stride=8), :] for i in range(2)]
        left = lax.broadcasted_iota(jnp.int32, one.shape, 1) < near
        turned_ref[rows, c * near : (c + 2) * near] = jnp.where(left, one, pltpu.roll(two, near, 1)).astype(BF16)
        turned_ref[beyond, c * near : (c + 2) * near] = jnp.where(left, pltpu.roll(one, near, 1), two).astype(BF16)


def offset_bits(sizes, group, j):
    groups = sizes[0] * sizes[1] * sizes[2] // GROUP
    last = group // (groups - 2)
    least = min if isinstance(group, int) else jnp.minimum
    first = 1 - least(group, 1)
    middle = 1 - last - first
    hot = middle * (group % 2) + last * (groups - 1 - group)
    which = middle * (group // 2 + 1) + last * (group - (groups - 2))
    width = sum((n - 1).bit_length() for n in sizes)
    return [j % 2, j // 2 % 2, hot] + [which // 2**k % 2 for k in range(width - 3)]


def peer_of(sizes, place, group, j):
    bits = offset_bits(sizes, group, j)
    at = list(place)
    for axis in (2, 1, 0):
        for k in range((sizes[axis] - 1).bit_length()):
            at[axis] = at[axis] + bits.pop(0) * (1 - place[axis] // 2**k % 2 * 2) * 2**k
    return tuple(at)


def place_batch(count, step, targets, carry, rank_ref, prefix_ref, row_ref, lane_ref):
    group = min(BATCH, max(1, CHUNK // count))
    groups, width, _ = splits(count)
    for inner in range(BATCH // group):
        masks, hots = [], []
        places = [
            pl.ds(pl.multiple_of((step * BATCH + inner * group + g) * CHUNK, CHUNK), CHUNK) for g in range(group)
        ]
        for at in places:
            mask = targets == jnp.broadcast_to(rank_ref[:, at], (count, CHUNK))
            masks.append(mask)
            hots.append(jnp.where(mask, 1.0, 0.0).astype(BF16))
        counted = jnp.dot(jnp.concatenate(hots, axis=0), prefix_ref[...], preferred_element_type=F32)
        for g, at in enumerate(places):
            piece = counted[g * count : (g + 1) * count]
            place_in = jnp.where(masks[g], piece[:, :CHUNK] + carry, 0.0)
            found = jnp.sum(place_in, axis=0, keepdims=True) - 1.0
            peer = jnp.floor(found * (1.0 / SPAN))
            position = found - peer * SPAN
            part = jnp.floor(position * (1.0 / width))
            block = jnp.floor(part * (1.0 / groups))
            lane_ref[:, at] = position - (part - block) * width
            row_ref[:, at] = (part - block * groups) * count + peer
            carry = carry + piece[:, CHUNK:]
    return carry


def route(
    sizes,
    place,
    blocks,
    loads,
    rank_ref,
    coords_ref,
    slot_ref,
    fields_ref,
    prefix_ref,
    turned_ref,
    flip_ref,
    row_ref,
    lane_ref,
    acc_ref,
):
    count = sizes[0] * sizes[1] * sizes[2]
    probes = slot_ref.shape[1]
    groups, width, per = splits(count)
    rows = groups * count
    spots = blocks * width
    tiles = fields_ref.shape[1] // LANES
    steps = probes // (BATCH * CHUNK)
    steps_of = lax.broadcasted_iota(jnp.int32, (count, CHUNK), 0)
    x, y, z = peer_of(sizes, place, steps_of // GROUP, steps_of % GROUP)
    targets = (x * sizes[1] + y) * sizes[2] + z
    row_ids = iota_bf16((rows, CHUNK))
    lane_ids = iota_bf16((spots, CHUNK))
    one, zero = jnp.ones((), BF16), jnp.zeros((), BF16)
    acc_ref[...] = jnp.zeros_like(acc_ref)

    def put(step, carry):
        return place_batch(count, step, targets, carry, rank_ref, prefix_ref, row_ref, lane_ref)

    def scatter(step):
        row_hots, lane_parts = [], []
        for g in range(BATCH):
            at = pl.ds(pl.multiple_of((step * BATCH + g) * CHUNK, CHUNK), CHUNK)
            row_hots.append(jnp.where(row_ids == spread(row_ref[:, at], rows), one, zero))
            here = lane_ids == spread(lane_ref[:, at], spots)
            parts = []
            slot = slot_ref[:, at]
            digits = [slot & 7, (slot >> 3) & 7, slot >> 6]
            for v in range(3):
                value = coords_ref[v : v + 1, at] * COARSE
                high = jnp.floor(value)
                low = jnp.floor((value - high) * FINE)
                parts += [high, low + (digits[v] * int(FINE) - int(COARSE)).astype(F32)]
            lane_parts.append(jnp.concatenate([jnp.where(here, spread(part, spots), zero) for part in parts], axis=0))
        acc_ref[...] += lax.dot_general(
            jnp.concatenate(lane_parts, axis=1),
            jnp.concatenate(row_hots, axis=1),
            (((1,), (1,)), ((), ())),
            preferred_element_type=F32,
        )
        for tile in range(tiles // steps):
            turn(step * (tiles // steps) + tile, fields_ref, turned_ref, flip_ref)

    def both(step, carry):
        scatter(step)
        return put(step + 1, carry)

    rank_ref[:, probes:] = jnp.zeros((1, rank_ref.shape[1] - probes), jnp.int32)
    loads[0].wait()
    carry = put(0, steps_of.astype(F32) * SPAN)
    for load in loads[1:]:
        load.wait()
    lax.fori_loop(0, steps, both, carry)


def assemble(count, blocks, acc_ref, send_ref, recv_ref):
    groups, width, per = splits(count)
    spots = blocks * width
    for b in range(blocks):
        for first in range(0, 4, per):
            stacked = []
            for half in range(groups // per):
                columns = slice(half * LANES, (half + 1) * LANES)
                values, slot = [], 0.0
                for v in range(3):
                    at = 2 * v * spots + b * width
                    high = acc_ref[at : at + width, columns]
                    low = acc_ref[at + spots : at + spots + width, columns] + COARSE
                    digit = jnp.floor(low * (1.0 / FINE))
                    values.append((high + (low - digit * FINE + 0.5) * (1.0 / FINE)) * (1.0 / COARSE))
                    slot = slot + digit * float(8**v)
                values.append(slot)
                pieces = values[first : first + per]
                stacked += exchange(pieces, count)
            flipped = jnp.concatenate(stacked, axis=0).T
            for v in range(first, first + per):
                send_ref[v * blocks + b] = flipped[(v - first) * count : (v - first + 1) * count]
                recv_ref[v * blocks + b, 0:1] = flipped[(v - first) * count : (v - first) * count + 1]


def lagrange(coord, nodes_ref):
    weight = nodes_ref[0:8, :]
    spread_coord = jnp.broadcast_to(coord, (8, LANES))
    for k in range(1, 8):
        weight = weight * (spread_coord - nodes_ref[8 * k : 8 * k + 8, :])
    return weight


def pick(blocks, block, first, recv_ref, nodes_ref, picker_ref):
    near = picker_ref.shape[0] // 8
    zero = jnp.zeros((), BF16)
    ids = iota_bf16((near, LANES))
    for j in range(GROUP):
        t, slot = [recv_ref[v * blocks + block, pl.ds(first + j, 1), :] for v in (2, 3)]
        weight_t = lagrange(t, nodes_ref)
        columns = slice(j * LANES, (j + 1) * LANES)
        mask = ids == spread(jnp.where(slot >= float(near), slot - float(near), slot), near)
        for c in range(8):
            picker_ref[c * near : (c + 1) * near, columns] = jnp.where(mask, spread(weight_t[c : c + 1, :], near), zero)


def combine(blocks, block, first, recv_ref, fields_ref, nodes_ref, values_ref, picker_ref):
    near = picker_ref.shape[0] // 8
    nodes = fields_ref.shape[0] // 2
    along = jnp.dot(fields_ref[...], picker_ref[...], preferred_element_type=F32)
    for j in range(GROUP):
        r, s, slot = [recv_ref[v * blocks + block, pl.ds(first + j, 1), :] for v in (0, 1, 3)]
        weight_r, weight_s = lagrange(r, nodes_ref), lagrange(s, nodes_ref)
        far = jnp.broadcast_to(slot, (8, LANES)) >= float(near)
        columns = slice(j * LANES, (j + 1) * LANES)
        factors = [jnp.broadcast_to(weight_r[a : a + 1, :], (8, LANES)) for a in range(8)]
        for f in range(4):
            total = None
            for a in range(8):
                at = f * 64 + a * 8
                here = jnp.where(far, along[nodes + at : nodes + at + 8, columns], along[at : at + 8, columns])
                total = here * factors[a] if a == 0 else total + here * factors[a]
            values_ref[f * blocks + block, pl.ds(first + j, 1), :] = jnp.sum(
                total * weight_s, axis=0, keepdims=True
            )


def sample_kernel(
    sizes,
    blocks,
    rank_in,
    coords_in,
    slot_in,
    fields_in,
    back_ref,
    row_ref,
    lane_ref,
    rank_ref,
    coords_ref,
    slot_ref,
    fields_ref,
    prefix_ref,
    nodes_ref,
    turned_ref,
    flip_ref,
    acc_ref,
    send_ref,
    recv_ref,
    values_ref,
    picker_even,
    picker_odd,
    out_sem,
    in_sem,
    back_out_sem,
    back_in_sem,
    load_sem,
):
    count = sizes[0] * sizes[1] * sizes[2]
    place = [lax.axis_index(axis) for axis in AXES]
    mesh_ids = pl.DeviceIdType.MESH

    def each(first, last, act):
        def body(step, _):
            act(step)
            return 0

        lax.fori_loop(first, last, body, 0)

    def outward(group, j):
        step = group * GROUP + j
        return pltpu.make_async_remote_copy(
            src_ref=send_ref.at[:, step],
            dst_ref=recv_ref.at[:, step],
            send_sem=out_sem.at[step],
            recv_sem=in_sem.at[step],
            device_id=peer_of(sizes, place, group, j),
            device_id_type=mesh_ids,
        )

    def backward(group, j):
        step = group * GROUP + j
        return pltpu.make_async_remote_copy(
            src_ref=values_ref.at[:, step],
            dst_ref=back_ref.at[:, step],
            send_sem=back_out_sem.at[step],
            recv_sem=back_in_sem.at[step],
            device_id=peer_of(sizes, place, group, j),
            device_id_type=mesh_ids,
        )

    loads = [
        pltpu.make_async_copy(source, target, load_sem.at[i])
        for i, (source, target) in enumerate(
            [(rank_in, rank_ref.at[:, : rank_in.shape[1]]), (coords_in, coords_ref), (slot_in, slot_ref), (fields_in, fields_ref)]
        )
    ]
    for load in loads:
        load.start()
    barrier = pltpu.get_barrier_semaphore()
    others = [(group, j) for group in range(count // GROUP) for j in range(GROUP) if group or j]
    for group, j in others:
        pl.semaphore_signal(barrier, inc=1, device_id=peer_of(sizes, place, group, j), device_id_type=mesh_ids)
    prepare(prefix_ref, nodes_ref)
    route(
        sizes,
        place,
        blocks,
        loads,
        rank_ref,
        coords_ref,
        slot_ref,
        fields_ref,
        prefix_ref,
        turned_ref,
        flip_ref,
        row_ref,
        lane_ref,
        acc_ref,
    )
    pl.semaphore_wait(barrier, count - 1)
    assemble(count, blocks, acc_ref, send_ref, recv_ref)
    groups = count // GROUP
    for group, j in others:
        outward(group, j).start()
    pickers = [picker_even, picker_odd]

    def serve(group):
        first = group * GROUP
        for block in range(blocks):
            pick(blocks, block, first, recv_ref, nodes_ref, pickers[block % 2])
            combine(blocks, block, first, recv_ref, turned_ref, nodes_ref, values_ref, pickers[block % 2])

    def body(group, _):
        @pl.when(group > 0)
        def _():
            outward(group, 0).wait_recv()

        for j in range(1, GROUP):
            outward(group, j).wait_recv()
        serve(group)
        for j in range(1, GROUP):
            backward(group, j).start()

        @pl.when(group > 0)
        def _():
            backward(group, 0).start()

        return 0

    lax.fori_loop(0, groups, body, 0)
    back_ref[:, 0:1] = values_ref[:, 0:1]

    def finish(group, skip):
        for j in range(skip, GROUP):
            outward(group, j).wait_send()
            backward(group, j).wait()

    def rest(group, _):
        finish(group, 0)
        return 0

    finish(0, 1)
    lax.fori_loop(1, groups, rest, 0)


def return_kernel(blocks, values_ref, row_ref, lane_ref, out_ref, table_ref):
    probes = out_ref.shape[1]
    count = values_ref.shape[1]
    groups, width, per = splits(count)
    rows = groups * count
    spots = blocks * width
    for b in range(blocks):
        for first in range(0, 4, per):
            stacked = [values_ref[f * blocks + b] for f in range(first, first + per)]
            flipped = jnp.concatenate(stacked, axis=0).T
            for half in range(groups // per):
                pieces = [flipped[(half * per + q) * width : (half * per + q + 1) * width] for q in range(per)]
                for f, piece in enumerate(exchange(pieces, count), first):
                    at = f * spots + b * width
                    table_ref[at : at + width, half * LANES : (half + 1) * LANES] = piece.astype(BF16)
    row_ids = iota_bf16((rows, CHUNK))
    lane_ids = lax.broadcasted_iota(jnp.int32, (spots, CHUNK), 0).astype(F32)

    def body(step, _):
        for g in range(SWEEP):
            at = pl.ds(pl.multiple_of((step * SWEEP + g) * CHUNK, CHUNK), CHUNK)
            hot = jnp.where(row_ids == spread(row_ref[:, at], rows), jnp.ones((), BF16), jnp.zeros((), BF16))
            picked = jnp.dot(table_ref[...], hot, preferred_element_type=F32)
            here = lane_ids == jnp.broadcast_to(lane_ref[:, at], (spots, CHUNK))
            for f in range(4):
                out_ref[f : f + 1, at] = jnp.sum(
                    jnp.where(here, picked[f * spots : (f + 1) * spots], 0.0), axis=0, keepdims=True
                )
        return 0

    lax.fori_loop(0, probes // (SWEEP * CHUNK), body, 0)


VMEM = pl.BlockSpec(memory_space=pltpu.VMEM)
HBM = pl.BlockSpec(memory_space=pltpu.HBM)


def call(kernel, inputs, outputs, scratch, **options):
    return pl.pallas_call(
        kernel,
        out_shape=outputs,
        in_specs=inputs,
        out_specs=jax.tree.map(lambda _: VMEM, outputs),
        scratch_shapes=scratch,
        compiler_params=pltpu.CompilerParams(vmem_limit_bytes=48 << 20, **options),
    )


def local(sizes, fields, coordinates, element_rank, element_slot):
    count = sizes[0] * sizes[1] * sizes[2]
    probes = element_slot.shape[0]
    elements = fields.shape[0]
    capacity = 5 * probes // (4 * count)
    blocks = -(-capacity // LANES)
    layout = jax.ShapeDtypeStruct((4 * blocks, count, LANES), F32)
    line = jax.ShapeDtypeStruct((1, probes + BATCH * CHUNK), F32)

    groups, width, _ = splits(count)
    spots, rows = blocks * width, groups * count
    depth = fields.shape[1] // 8
    picker = pltpu.VMEM((4 * elements, GROUP * LANES), BF16)
    buffer = pltpu.VMEM(layout.shape, F32)
    arrivals = pltpu.SemaphoreType.DMA((count,))
    returned, row, lane = call(
        functools.partial(sample_kernel, sizes, blocks),
        [HBM] * 4,
        (layout, line, line),
        [
            pltpu.VMEM(line.shape, jnp.int32),
            pltpu.VMEM((3, probes), F32),
            pltpu.VMEM((1, probes), jnp.int32),
            pltpu.VMEM(fields.shape, BF16),
            pltpu.VMEM((CHUNK, 2 * CHUNK), BF16),
            pltpu.VMEM((64, LANES), F32),
            pltpu.VMEM((2 * depth, 4 * elements), BF16),
            pltpu.VMEM((LANES, elements), F32),
            pltpu.VMEM((6 * spots, rows), F32),
        ]
        + [buffer] * 3
        + [picker] * 2
        + [arrivals] * 4
        + [pltpu.SemaphoreType.DMA((4,))],
        collective_id=0,
        has_side_effects=True,
    )(
        *[
            pltpu.with_memory_space_constraint(x, pltpu.HBM)
            for x in (element_rank.reshape(1, probes), coordinates, element_slot.reshape(1, probes), fields)
        ]
    )
    return call(
        functools.partial(return_kernel, blocks),
        [VMEM] * 3,
        jax.ShapeDtypeStruct((4, probes), F32),
        [pltpu.VMEM((4 * spots, rows), BF16)],
    )(returned, row, lane)


def solution(mesh):
    sizes = tuple(mesh.shape[axis] for axis in AXES)
    placed = (P(AXES, None), P(None, AXES), P(AXES, None), P(AXES))
    return jax.shard_map(
        functools.partial(local, sizes),
        mesh=mesh,
        in_specs=placed,
        out_specs=P(None, AXES),
        check_vma=False,
    )
```

```python
import functools

import jax
import jax.numpy as jnp
import numpy as np
from jax import lax
from jax.experimental import pallas as pl
from jax.experimental.pallas import tpu as pltpu
from jax.sharding import PartitionSpec as P

AXES = ("gx", "gy", "gz")
F32, BF16 = jnp.float32, jnp.bfloat16
LANES = 128
CHUNK = 256
GROUP = 4
BATCH = 16
SWEEP = 32
SPAN = 1024.0
COARSE = 256.0
FINE = 64.0

gll_points = np.array(
    [
        -1.0,
        -0.8717401485096066,
        -0.5917001814331423,
        -0.2092992179024789,
        0.2092992179024789,
        0.5917001814331423,
        0.8717401485096066,
        1.0,
    ]
)
gll_scale = np.array(
    [1.0 / np.prod([gll_points[a] - gll_points[b] for b in range(8) if b != a]) for a in range(8)]
)


def column(values):
    node = lax.broadcasted_iota(jnp.int32, (8, LANES), 0)
    out = jnp.full((8, LANES), float(values[0]), F32)
    for a in range(1, 8):
        out = jnp.where(node == a, float(values[a]), out)
    return out


def iota_bf16(shape):
    return lax.broadcasted_iota(jnp.int32, shape, 0).astype(F32).astype(BF16)


def spread(row, count):
    return jnp.broadcast_to(row, (count, row.shape[1])).astype(BF16)


def splits(count):
    groups = max(1, 2 * LANES // count)
    return groups, LANES // groups, max(1, LANES // count)


def exchange(pieces, count):
    block = lax.broadcasted_iota(jnp.int32, pieces[0].shape, 1) // count
    bit = len(pieces) // 2
    while bit:
        high = (block // bit) % 2 == 1
        swapped = []
        for i, own in enumerate(pieces):
            upper = (i // bit) % 2 == 1
            other = pltpu.roll(pieces[i - bit if upper else i + bit], LANES - bit * count if upper else bit * count, 1)
            swapped.append(jnp.where(high, own, other) if upper else jnp.where(high, other, own))
        pieces = swapped
        bit //= 2
    return pieces


def prepare(prefix_ref, nodes_ref):
    below = lax.broadcasted_iota(jnp.int32, (CHUNK, CHUNK), 0) <= lax.broadcasted_iota(jnp.int32, (CHUNK, CHUNK), 1)
    prefix_ref[:, :CHUNK] = jnp.where(below, 1.0, 0.0).astype(BF16)
    prefix_ref[:, CHUNK:] = jnp.ones((CHUNK, CHUNK), BF16)
    nodes_ref[0:8, :] = column(gll_scale)
    for k in range(1, 8):
        nodes_ref[8 * k : 8 * k + 8, :] = column(np.roll(gll_points, -k))


def turn(tile, fields_ref, turned_ref, flip_ref):
    elements = fields_ref.shape[0]
    columns = pl.ds(pl.multiple_of(tile * LANES, LANES), LANES)
    rows = pl.ds(pl.multiple_of(tile * 16, 16), 16)
    flip_ref[...] = fields_ref[:, columns].astype(F32).T
    near, nodes = elements // 2, turned_ref.shape[0] // 2
    beyond = pl.ds(pl.multiple_of(nodes + tile * 16, 16), 16)
    for c in range(0, 8, 2):
        one, two = [flip_ref[pl.ds(c + i, 16, stride=8), :] for i in range(2)]
        left = lax.broadcasted_iota(jnp.int32, one.shape, 1) < near
        turned_ref[rows, c * near : (c + 2) * near] = jnp.where(left, one, pltpu.roll(two, near, 1)).astype(BF16)
        turned_ref[beyond, c * near : (c + 2) * near] = jnp.where(left, pltpu.roll(one, near, 1), two).astype(BF16)


def offset_bits(sizes, group, j):
    groups = sizes[0] * sizes[1] * sizes[2] // GROUP
    last = group // (groups - 2)
    least = min if isinstance(group, int) else jnp.minimum
    first = 1 - least(group, 1)
    middle = 1 - last - first
    hot = middle * (group % 2) + last * (groups - 1 - group)
    which = middle * (group // 2 + 1) + last * (group - (groups - 2))
    width = sum((n - 1).bit_length() for n in sizes)
    return [j % 2, j // 2 % 2, hot] + [which // 2**k % 2 for k in range(width - 3)]


def peer_of(sizes, place, group, j):
    bits = offset_bits(sizes, group, j)
    at = list(place)
    for axis in (2, 1, 0):
        for k in range((sizes[axis] - 1).bit_length()):
            at[axis] = at[axis] + bits.pop(0) * (1 - place[axis] // 2**k % 2 * 2) * 2**k
    return tuple(at)


def place_batch(count, step, targets, carry, rank_ref, prefix_ref, row_ref, lane_ref, next_ref):
    group = min(BATCH, max(1, CHUNK // count))
    groups, width, _ = splits(count)
    for inner in range(BATCH // group):
        masks, hots = [], []
        places = [
            pl.ds(pl.multiple_of((step * BATCH + inner * group + g) * CHUNK, CHUNK), CHUNK) for g in range(group)
        ]
        for at in places:
            mask = targets == jnp.broadcast_to(rank_ref[:, at], (count, CHUNK))
            masks.append(mask)
            hots.append(jnp.where(mask, 1.0, 0.0).astype(BF16))
        counted = jnp.dot(jnp.concatenate(hots, axis=0), prefix_ref[...], preferred_element_type=F32)
        for g, at in enumerate(places):
            piece = counted[g * count : (g + 1) * count]
            place_in = jnp.where(masks[g], piece[:, :CHUNK] + carry, 0.0)
            found = jnp.sum(place_in, axis=0, keepdims=True) - 1.0
            peer = jnp.floor(found * (1.0 / SPAN))
            position = found - peer * SPAN
            part = jnp.floor(position * (1.0 / width))
            block = jnp.floor(part * (1.0 / groups))
            lane = position - (part - block) * width
            row = (part - block * groups) * count + peer
            lane_ref[:, at] = lane
            row_ref[:, at] = row
            here = slice((inner * group + g) * CHUNK, (inner * group + g + 1) * CHUNK)
            next_ref[0, :, here] = row
            next_ref[1, :, here] = lane
            carry = carry + piece[:, CHUNK:]
    return carry


def route(
    sizes,
    place,
    blocks,
    loads,
    rank_ref,
    coords_ref,
    slot_ref,
    fields_ref,
    prefix_ref,
    turned_ref,
    flip_ref,
    row_ref,
    lane_ref,
    next_ref,
    now_ref,
    acc_ref,
):
    count = sizes[0] * sizes[1] * sizes[2]
    probes = slot_ref.shape[1]
    groups, width, per = splits(count)
    rows = groups * count
    spots = blocks * width
    tiles = fields_ref.shape[1] // LANES
    steps = probes // (BATCH * CHUNK)
    steps_of = lax.broadcasted_iota(jnp.int32, (count, CHUNK), 0)
    x, y, z = peer_of(sizes, place, steps_of // GROUP, steps_of % GROUP)
    targets = (x * sizes[1] + y) * sizes[2] + z
    row_ids = iota_bf16((rows, CHUNK))
    lane_ids = iota_bf16((spots, CHUNK))
    one, zero = jnp.ones((), BF16), jnp.zeros((), BF16)
    acc_ref[...] = jnp.zeros_like(acc_ref)

    def put(step, carry):
        return place_batch(count, step, targets, carry, rank_ref, prefix_ref, row_ref, lane_ref, next_ref)

    def scatter(step):
        row_hots, lane_parts = [], []
        for g in range(BATCH):
            at = pl.ds(pl.multiple_of((step * BATCH + g) * CHUNK, CHUNK), CHUNK)
            here = slice(g * CHUNK, (g + 1) * CHUNK)
            row_hots.append(jnp.where(row_ids == spread(now_ref[0, :, here], rows), one, zero))
            inside = lane_ids == spread(now_ref[1, :, here], spots)
            parts = []
            slot = slot_ref[:, at]
            digits = [slot & 7, (slot >> 3) & 7, slot >> 6]
            for v in range(3):
                value = coords_ref[v : v + 1, at] * COARSE
                high = jnp.floor(value)
                low = jnp.floor((value - high) * FINE)
                parts += [high, low + (digits[v] * int(FINE) - int(COARSE)).astype(F32)]
            lane_parts.append(jnp.concatenate([jnp.where(inside, spread(part, spots), zero) for part in parts], axis=0))
        acc_ref[...] += lax.dot_general(
            jnp.concatenate(lane_parts, axis=1),
            jnp.concatenate(row_hots, axis=1),
            (((1,), (1,)), ((), ())),
            preferred_element_type=F32,
        )
        for tile in range(tiles // steps):
            turn(step * (tiles // steps) + tile, fields_ref, turned_ref, flip_ref)

    def both(step, carry):
        carry = put(step + 1, carry)
        scatter(step)
        now_ref[...] = next_ref[...]
        return carry

    rank_ref[:, probes:] = jnp.zeros((1, rank_ref.shape[1] - probes), jnp.int32)
    loads[0].wait()
    carry = put(0, steps_of.astype(F32) * SPAN)
    now_ref[...] = next_ref[...]
    for load in loads[1:]:
        load.wait()
    lax.fori_loop(0, steps, both, carry)


def assemble(count, blocks, acc_ref, send_ref, recv_ref):
    groups, width, per = splits(count)
    spots = blocks * width
    for b in range(blocks):
        for first in range(0, 4, per):
            stacked = []
            for half in range(groups // per):
                columns = slice(half * LANES, (half + 1) * LANES)
                values, slot = [], 0.0
                for v in range(3):
                    at = 2 * v * spots + b * width
                    high = acc_ref[at : at + width, columns]
                    low = acc_ref[at + spots : at + spots + width, columns] + COARSE
                    digit = jnp.floor(low * (1.0 / FINE))
                    values.append((high + (low - digit * FINE + 0.5) * (1.0 / FINE)) * (1.0 / COARSE))
                    slot = slot + digit * float(8**v)
                values.append(slot)
                pieces = values[first : first + per]
                stacked += exchange(pieces, count)
            flipped = jnp.concatenate(stacked, axis=0).T
            for v in range(first, first + per):
                send_ref[v * blocks + b] = flipped[(v - first) * count : (v - first + 1) * count]
                recv_ref[v * blocks + b, 0:1] = flipped[(v - first) * count : (v - first) * count + 1]


def lagrange(coord, nodes_ref):
    weight = nodes_ref[0:8, :]
    spread_coord = jnp.broadcast_to(coord, (8, LANES))
    for k in range(1, 8):
        weight = weight * (spread_coord - nodes_ref[8 * k : 8 * k + 8, :])
    return weight


def pick(blocks, block, first, recv_ref, nodes_ref, picker_ref):
    near = picker_ref.shape[0] // 8
    zero = jnp.zeros((), BF16)
    ids = iota_bf16((near, LANES))
    for j in range(GROUP):
        t, slot = [recv_ref[v * blocks + block, pl.ds(first + j, 1), :] for v in (2, 3)]
        weight_t = lagrange(t, nodes_ref)
        columns = slice(j * LANES, (j + 1) * LANES)
        mask = ids == spread(jnp.where(slot >= float(near), slot - float(near), slot), near)
        for c in range(8):
            picker_ref[c * near : (c + 1) * near, columns] = jnp.where(mask, spread(weight_t[c : c + 1, :], near), zero)


def combine(blocks, block, first, recv_ref, fields_ref, nodes_ref, values_ref, picker_ref):
    near = picker_ref.shape[0] // 8
    nodes = fields_ref.shape[0] // 2
    along = jnp.dot(fields_ref[...], picker_ref[...], preferred_element_type=F32)
    for j in range(GROUP):
        r, s, slot = [recv_ref[v * blocks + block, pl.ds(first + j, 1), :] for v in (0, 1, 3)]
        weight_r, weight_s = lagrange(r, nodes_ref), lagrange(s, nodes_ref)
        far = jnp.broadcast_to(slot, (8, LANES)) >= float(near)
        columns = slice(j * LANES, (j + 1) * LANES)
        factors = [jnp.broadcast_to(weight_r[a : a + 1, :], (8, LANES)) for a in range(8)]
        for f in range(4):
            total = None
            for a in range(8):
                at = f * 64 + a * 8
                here = jnp.where(far, along[nodes + at : nodes + at + 8, columns], along[at : at + 8, columns])
                total = here * factors[a] if a == 0 else total + here * factors[a]
            values_ref[f * blocks + block, pl.ds(first + j, 1), :] = jnp.sum(
                total * weight_s, axis=0, keepdims=True
            )


def sample_kernel(
    sizes,
    blocks,
    rank_in,
    coords_in,
    slot_in,
    fields_in,
    back_ref,
    row_ref,
    lane_ref,
    rank_ref,
    coords_ref,
    slot_ref,
    fields_ref,
    prefix_ref,
    nodes_ref,
    turned_ref,
    flip_ref,
    next_ref,
    now_ref,
    acc_ref,
    send_ref,
    recv_ref,
    values_ref,
    picker_even,
    picker_odd,
    out_sem,
    in_sem,
    back_out_sem,
    back_in_sem,
    load_sem,
):
    count = sizes[0] * sizes[1] * sizes[2]
    place = [lax.axis_index(axis) for axis in AXES]
    mesh_ids = pl.DeviceIdType.MESH

    def each(first, last, act):
        def body(step, _):
            act(step)
            return 0

        lax.fori_loop(first, last, body, 0)

    def outward(group, j):
        step = group * GROUP + j
        return pltpu.make_async_remote_copy(
            src_ref=send_ref.at[:, step],
            dst_ref=recv_ref.at[:, step],
            send_sem=out_sem.at[step],
            recv_sem=in_sem.at[step],
            device_id=peer_of(sizes, place, group, j),
            device_id_type=mesh_ids,
        )

    def backward(group, j):
        step = group * GROUP + j
        return pltpu.make_async_remote_copy(
            src_ref=values_ref.at[:, step],
            dst_ref=back_ref.at[:, step],
            send_sem=back_out_sem.at[step],
            recv_sem=back_in_sem.at[step],
            device_id=peer_of(sizes, place, group, j),
            device_id_type=mesh_ids,
        )

    loads = [
        pltpu.make_async_copy(source, target, load_sem.at[i])
        for i, (source, target) in enumerate(
            [(rank_in, rank_ref.at[:, : rank_in.shape[1]]), (coords_in, coords_ref), (slot_in, slot_ref), (fields_in, fields_ref)]
        )
    ]
    for load in loads:
        load.start()
    barrier = pltpu.get_barrier_semaphore()
    others = [(group, j) for group in range(count // GROUP) for j in range(GROUP) if group or j]
    for group, j in others:
        pl.semaphore_signal(barrier, inc=1, device_id=peer_of(sizes, place, group, j), device_id_type=mesh_ids)
    prepare(prefix_ref, nodes_ref)
    route(
        sizes,
        place,
        blocks,
        loads,
        rank_ref,
        coords_ref,
        slot_ref,
        fields_ref,
        prefix_ref,
        turned_ref,
        flip_ref,
        row_ref,
        lane_ref,
        next_ref,
        now_ref,
        acc_ref,
    )
    pl.semaphore_wait(barrier, count - 1)
    assemble(count, blocks, acc_ref, send_ref, recv_ref)
    groups = count // GROUP
    for group, j in others:
        outward(group, j).start()
    pickers = [picker_even, picker_odd]

    def serve(group):
        first = group * GROUP
        for block in range(blocks):
            pick(blocks, block, first, recv_ref, nodes_ref, pickers[block % 2])
            combine(blocks, block, first, recv_ref, turned_ref, nodes_ref, values_ref, pickers[block % 2])

    def body(group, _):
        @pl.when(group > 0)
        def _():
            outward(group, 0).wait_recv()

        for j in range(1, GROUP):
            outward(group, j).wait_recv()
        serve(group)
        for j in range(1, GROUP):
            backward(group, j).start()

        @pl.when(group > 0)
        def _():
            backward(group, 0).start()

        return 0

    lax.fori_loop(0, groups, body, 0)
    back_ref[:, 0:1] = values_ref[:, 0:1]

    def finish(group, skip):
        for j in range(skip, GROUP):
            outward(group, j).wait_send()
            backward(group, j).wait()

    def rest(group, _):
        finish(group, 0)
        return 0

    finish(0, 1)
    lax.fori_loop(1, groups, rest, 0)


def return_kernel(blocks, values_ref, row_ref, lane_ref, out_ref, table_ref):
    probes = out_ref.shape[1]
    count = values_ref.shape[1]
    groups, width, per = splits(count)
    rows = groups * count
    spots = blocks * width
    for b in range(blocks):
        for first in range(0, 4, per):
            stacked = [values_ref[f * blocks + b] for f in range(first, first + per)]
            flipped = jnp.concatenate(stacked, axis=0).T
            for half in range(groups // per):
                pieces = [flipped[(half * per + q) * width : (half * per + q + 1) * width] for q in range(per)]
                for f, piece in enumerate(exchange(pieces, count), first):
                    at = f * spots + b * width
                    table_ref[at : at + width, half * LANES : (half + 1) * LANES] = piece.astype(BF16)
    row_ids = iota_bf16((rows, CHUNK))
    lane_ids = lax.broadcasted_iota(jnp.int32, (spots, CHUNK), 0).astype(F32)

    def body(step, _):
        for g in range(SWEEP):
            at = pl.ds(pl.multiple_of((step * SWEEP + g) * CHUNK, CHUNK), CHUNK)
            hot = jnp.where(row_ids == spread(row_ref[:, at], rows), jnp.ones((), BF16), jnp.zeros((), BF16))
            picked = jnp.dot(table_ref[...], hot, preferred_element_type=F32)
            here = lane_ids == jnp.broadcast_to(lane_ref[:, at], (spots, CHUNK))
            for f in range(4):
                out_ref[f : f + 1, at] = jnp.sum(
                    jnp.where(here, picked[f * spots : (f + 1) * spots], 0.0), axis=0, keepdims=True
                )
        return 0

    lax.fori_loop(0, probes // (SWEEP * CHUNK), body, 0)


VMEM = pl.BlockSpec(memory_space=pltpu.VMEM)
HBM = pl.BlockSpec(memory_space=pltpu.HBM)


def call(kernel, inputs, outputs, scratch, **options):
    return pl.pallas_call(
        kernel,
        out_shape=outputs,
        in_specs=inputs,
        out_specs=jax.tree.map(lambda _: VMEM, outputs),
        scratch_shapes=scratch,
        compiler_params=pltpu.CompilerParams(vmem_limit_bytes=48 << 20, **options),
    )


def local(sizes, fields, coordinates, element_rank, element_slot):
    count = sizes[0] * sizes[1] * sizes[2]
    probes = element_slot.shape[0]
    elements = fields.shape[0]
    capacity = 5 * probes // (4 * count)
    blocks = -(-capacity // LANES)
    layout = jax.ShapeDtypeStruct((4 * blocks, count, LANES), F32)
    line = jax.ShapeDtypeStruct((1, probes + BATCH * CHUNK), F32)

    groups, width, _ = splits(count)
    spots, rows = blocks * width, groups * count
    depth = fields.shape[1] // 8
    picker = pltpu.VMEM((4 * elements, GROUP * LANES), BF16)
    buffer = pltpu.VMEM(layout.shape, F32)
    arrivals = pltpu.SemaphoreType.DMA((count,))
    returned, row, lane = call(
        functools.partial(sample_kernel, sizes, blocks),
        [HBM] * 4,
        (layout, line, line),
        [
            pltpu.VMEM(line.shape, jnp.int32),
            pltpu.VMEM((3, probes), F32),
            pltpu.VMEM((1, probes), jnp.int32),
            pltpu.VMEM(fields.shape, BF16),
            pltpu.VMEM((CHUNK, 2 * CHUNK), BF16),
            pltpu.VMEM((64, LANES), F32),
            pltpu.VMEM((2 * depth, 4 * elements), BF16),
            pltpu.VMEM((LANES, elements), F32),
            pltpu.VMEM((2, 1, BATCH * CHUNK), F32),
            pltpu.VMEM((2, 1, BATCH * CHUNK), F32),
            pltpu.VMEM((6 * spots, rows), F32),
        ]
        + [buffer] * 3
        + [picker] * 2
        + [arrivals] * 4
        + [pltpu.SemaphoreType.DMA((4,))],
        collective_id=0,
        has_side_effects=True,
    )(
        *[
            pltpu.with_memory_space_constraint(x, pltpu.HBM)
            for x in (element_rank.reshape(1, probes), coordinates, element_slot.reshape(1, probes), fields)
        ]
    )
    return call(
        functools.partial(return_kernel, blocks),
        [VMEM] * 3,
        jax.ShapeDtypeStruct((4, probes), F32),
        [pltpu.VMEM((4 * spots, rows), BF16)],
    )(returned, row, lane)


def solution(mesh):
    sizes = tuple(mesh.shape[axis] for axis in AXES)
    placed = (P(AXES, None), P(None, AXES), P(AXES, None), P(AXES))
    return jax.shard_map(
        functools.partial(local, sizes),
        mesh=mesh,
        in_specs=placed,
        out_specs=P(None, AXES),
        check_vma=False,
    )
```
